32 devices in a mesh: bank: 4 (over x, core), lane: 8 (over z, y).
Axes of the slice: x: 2, y: 2, z: 4, core: 2. Of those that a mesh axis runs over, the one named last changes fastest.
Arguments:
- amplitudes: float32 [2, 512, 128, 128], P(None, ('bank', 'lane')), may hold values from -6 to 6
- energies: float32 [512, 128, 128], P(('bank', 'lane')), may hold values from -2 to 2
- diagonal_angles: float32 [2, 128], replicated, may hold values from 0.3 to 1.2
- turn_angles: float32 [2, 4], replicated, may hold values from 0.3 to 1.2
Outputs:
- state_after: float32 [2, 512, 128, 128], P(None, ('bank', 'lane'))
The draws below stay inside these ranges and needn't reach their ends.
All inputs are finite; a program needn't handle non-finite values.
Results may differ from the reference program's by a relative error of at most 0.0003.
Values sent between devices are 32-bit elements; how exact they have to be, the bound alone decides.
A program may use at most 64 MiB of HBM per device.

```python
import jax
import jax.numpy as jnp
from jax import lax

BLOCKS_DEV = 16
ROWS = 128
LANES = 128
BLOCKS = 512
LAYERS = 2
N_BANK = 4
N_LANE = 8


def shard_levels(key, dims, cuts, smallest, high):
    def one(axis_at, blocks):
        heights = jax.random.uniform(jax.random.fold_in(jax.random.fold_in(key, 6), axis_at), (blocks,), jnp.float32, smallest / len(cuts), high / len(cuts))
        return jnp.repeat(jnp.exp(heights), dims[axis_at] // blocks).reshape((-1,) + (1,) * (len(dims) - axis_at - 1))

    loudness = one(*cuts[0])
    for cut in cuts[1:]:
        loudness = loudness * one(*cut)
    return loudness


def gaussian(own_key, extent, width, most, cuts=(), held_as=jnp.bfloat16):
    drawn = width * jax.random.normal(own_key, extent, jnp.float32)
    if cuts:
        drawn = drawn * shard_levels(own_key, extent, cuts, -0.22, 0.18)
    return jnp.clip(drawn, -most, most).astype(held_as)


def setup_inputs(seed: int = 0) -> dict:
    splits = jax.random.split(jax.random.key(seed), 5)
    amplitudes = gaussian(splits[0], (2, BLOCKS, ROWS, LANES), 1.0, 6.0, ((1, 32),), jnp.float32)
    energies = jnp.clip(jax.random.uniform(splits[1], (BLOCKS, ROWS, LANES), jnp.float32, -2.0, 2.0) * shard_levels(splits[1], (BLOCKS, ROWS, LANES), ((0, 32),), -0.4, 0.0), -2.0, 2.0)
    diagonal_angles = jnp.clip(jax.random.uniform(splits[2], (LAYERS, LANES), jnp.float32, 0.3, 1.2), 0.3, 1.2)
    turn_angles = jnp.clip(jax.random.uniform(splits[3], (LAYERS, 4), jnp.float32, 0.3, 1.2), 0.3, 1.2)
    return {"amplitudes": amplitudes, "energies": energies, "diagonal_angles": diagonal_angles, "turn_angles": turn_angles}


def count_bits(values, count):
    places = jnp.arange(count.bit_length() - 1, dtype=jnp.int32)
    return jnp.sum((values[..., None] >> places) & 1, axis=-1)


def plane_table(count, angle):
    rank = jnp.arange(count, dtype=jnp.int32)
    apart = count_bits(rank[:, None] ^ rank[None, :], count)
    minus = count_bits(rank[:, None] & (rank[:, None] ^ rank[None, :]), count)
    bits = count.bit_length() - 1
    size = jnp.cos(angle) ** (bits - apart).astype(jnp.float32) * jnp.sin(angle) ** apart.astype(jnp.float32)
    return size * jnp.where(minus % 2 == 1, -1.0, 1.0).astype(jnp.float32)


def mix_dim(values, dim, angle):
    real_part = plane_table(values.shape[dim], angle)
    def times(table):
        moved = jnp.tensordot(values, table, axes=([dim], [0]), precision=lax.Precision.HIGHEST)
        return jnp.moveaxis(moved, -1, dim)
    return times(real_part)


def phase_step(values, levels, angle):
    turn = angle * levels
    return jnp.stack([values[0] * jnp.cos(turn) + values[1] * jnp.sin(turn), values[1] * jnp.cos(turn) - values[0] * jnp.sin(turn)])


def reference(amplitudes, energies, diagonal_angles, turn_angles):
    values = amplitudes
    for layer in range(LAYERS):
        values = phase_step(values, energies, diagonal_angles[layer])
        values = mix_dim(values, 3, turn_angles[layer, 0])
        values = mix_dim(values, 2, turn_angles[layer, 1])
        parts = values.reshape(2, N_BANK, N_LANE, BLOCKS_DEV, ROWS, LANES)
        parts = mix_dim(parts, 1, turn_angles[layer, 2])
        parts = mix_dim(parts, 2, turn_angles[layer, 3])
        parts = mix_dim(parts, 3, turn_angles[layer, 2])
        values = parts.reshape(values.shape)
    return values
```

```python
import functools
import math

import jax
import jax.numpy as jnp
from jax import lax
from jax.experimental import pallas as pl
from jax.experimental.pallas import tpu as pltpu
from jax.sharding import PartitionSpec as P

LAYERS = 2
VMEM_MOST = 67043328
ROOM = 1 << 18
MESH = pl.DeviceIdType.MESH
SUB = 8
ROWS_SLAB = 16


def bits_of(count):
    return count.bit_length() - 1


def xor(number, mask, count):
    out = 0
    for place in range(bits_of(count)):
        weight = 1 << place
        one = lax.rem(lax.div(number, weight), 2) + lax.rem(lax.div(mask, weight), 2)
        out = out + lax.rem(one, 2) * weight
    return out


def flips(number, count):
    out = [number]
    for place in range(bits_of(count)):
        weight = 1 << place
        change = weight - 2 * weight * lax.rem(lax.div(number, weight), 2)
        out = out + [other + change for other in out]
    return out


def cos_sin(turn):
    half = 0.5 * turn
    square = half * half
    sine = jnp.full_like(half, -1.0 / math.factorial(11))
    for power in (9, 7, 5, 3, 1):
        sine = sine * square + (-1.0) ** (power // 2) / math.factorial(power)
    sine = sine * half
    cosine = jnp.full_like(half, -1.0 / math.factorial(10))
    for power in (8, 6, 4, 2, 0):
        cosine = cosine * square + (-1.0) ** (power // 2) / math.factorial(power)
    double = sine + sine
    return 1.0 - double * sine, double * cosine


def turned(pieces, slope, low, high):
    pieces = list(pieces)
    for place in range(low, high):
        step = 1 << place
        for at in range(len(pieces)):
            if not at & step:
                u, v = pieces[at], pieces[at + step]
                pieces[at], pieces[at + step] = u - slope * v, v + slope * u
    return pieces


def mix_slabs(values, mixed, tangent):
    slabs, rows, _ = values.shape
    places = [(s, slice(e, e + SUB)) for s in range(slabs) for e in range(0, rows, SUB)]
    pieces = [values[s, e, :] for s, e in places]
    pieces = turned(pieces, tangent, 0, bits_of(len(places)))
    for (s, e), piece in zip(places, pieces):
        mixed[s, e, :] = piece


def finish(values, tangent, out_hbm, mixed, sem):
    _, blocks, groups, _, _, _ = values.shape

    def one(b, carry):
        for part in range(2):
            for g in range(groups):
                mix_slabs(values.at[part, b, g], mixed.at[part, b, g], tangent[...])
        pltpu.make_async_copy(mixed.at[:, b], out_hbm.at[:, b], sem).start()
        return carry

    lax.fori_loop(0, blocks, one, 0)
    pltpu.make_async_copy(mixed, out_hbm, sem).wait()


def kernel(
    nb, nl, amp_hbm, en_hbm, diag_hbm, turn_hbm, out, last,
    amp, en, diag_ref, turn_ref, rs, re, back, table, slope, signed,
    in_sem, s_send, s_recv, e_send, e_recv, b_send, b_recv, side, outer_in, inner_in, here, all_in,
):
    _, blocks, groups, slabs, rows, lanes = amp.shape
    devices = nb * nl
    others = devices - 1
    eights = rows // SUB
    me_b, me_l = lax.axis_index("bank"), lax.axis_index("lane")
    me = me_b * nl + me_l
    my_block, my_group = lax.rem(me, blocks), lax.div(me, blocks)

    load_en = pltpu.make_async_copy(en_hbm, en, in_sem.at[0])
    load_en.start()
    load_turn = pltpu.make_async_copy(turn_hbm, turn_ref, in_sem.at[2])
    load_turn.start()
    load_diag = pltpu.make_async_copy(diag_hbm, diag_ref, in_sem.at[3])
    load_diag.start()
    load_amp = pltpu.make_async_copy(amp_hbm, amp, in_sem.at[1])
    load_amp.start()

    flip_b = flips(me_b, nb)
    flip_l = flips(me_l, nl)

    high, low = nl // 2, nl // 4
    mirror = high + low
    inner = lax.rem(lax.div(me_l, high), 2) != lax.rem(lax.div(me_l, low), 2)
    sides = [(1 << place, 0) for place in range(bits_of(nb))]
    sides += [(0, 1 << place) for place in range(bits_of(low))]
    mirrored = devices // 4
    unmirrored = others - mirrored

    def signal(sem, flip):
        pl.semaphore_signal(
            sem, inc=1, device_id=(flip_b[flip[0]], flip_l[flip[1]]), device_id_type=MESH
        )

    def to_unmirrored(action):
        def step(i, carry):
            k = unmirrored - i
            db, dl = xor(me_b, lax.rem(k, nb), nb), xor(me_l, lax.div(k, nb), nl)
            action(db, dl, db * nl + dl)
            return carry

        lax.fori_loop(0, unmirrored, step, 0)

    def to_peers(lane_flips, action):
        for flip in lane_flips:
            far_first = flip - low if flip & low else flip + low
            mine = jnp.where(inner, far_first, flip) if flip & high else flip
            dl = xor(me_l, mine, nl)

            def step(i, carry):
                db = xor(me_b, nb - 1 - i, nb)
                action(db, dl, db * nl + dl)
                return carry

            lax.fori_loop(0, nb if flip else nb - 1, step, 0)

    crossing_first = list(range(nl - 1, -1, -1))
    in_turn = [flip for at in range(high - 1, -1, -1) for flip in (high + at, at)]

    barrier = pltpu.get_barrier_semaphore()

    def send_en(low_slab, count, at, each):
        def one(db, dl, d):
            pltpu.make_async_remote_copy(
                src_ref=en.at[lax.rem(d, blocks), lax.div(d, blocks), pl.ds(low_slab, count)],
                dst_ref=re.at[me, pl.ds(low_slab, count)],
                send_sem=e_send.at[at],
                recv_sem=e_recv.at[at],
                device_id=(db, dl),
                device_id_type=MESH,
            ).start()

        each(one)

    def send_en_mirrored(found):
        def each(action):
            for bank_flip, lane_flip in found:
                db, dl = flip_b[bank_flip], flip_l[lane_flip + mirror]
                action(db, dl, db * nl + dl)

        send_en(0, slabs, 2, each)

    @pl.when(inner)
    def _():
        for flip in [(0, mirror)] + sides + [(0, low)]:
            signal(barrier, flip)
        pl.semaphore_wait(barrier, 1 + len(sides))
        load_en.wait()
        found = [(0, 0)]
        send_en_mirrored(found)
        for at, flip in enumerate(sides):
            signal(side.at[at], flip)
            pl.semaphore_wait(side.at[at], 1)
            more = [(b + flip[0], l + flip[1]) for b, l in found]
            send_en_mirrored(more)
            found += more
        pl.semaphore_wait(outer_in, 1)
        signal(inner_in, (0, low))

    @pl.when(jnp.logical_not(inner))
    def _():
        pl.semaphore_wait(barrier, 1)
        signal(outer_in, (0, low))
        load_en.wait()
        pl.semaphore_wait(inner_in, 1)
        for lane_flip in list(range(high, mirror)) + list(range(low, high)):
            for bank_flip in range(nb):
                signal(here, (bank_flip, lane_flip))

    def meet_all():
        @pl.when(inner)
        def _():
            pl.semaphore_wait(here, devices // 2)
            signal(all_in, (0, low))

        @pl.when(jnp.logical_not(inner))
        def _():
            pl.semaphore_wait(all_in, 1)
            send_en_mirrored([(b, l) for l in range(low) for b in range(nb)])

        send_en(0, 1, 0, to_unmirrored)

    def send_state(s):
        def one(db, dl, d):
            pltpu.make_async_remote_copy(
                src_ref=amp.at[:, lax.rem(d, blocks), lax.div(d, blocks), s],
                dst_ref=rs.at[me, :, s],
                send_sem=s_send.at[s],
                recv_sem=s_recv.at[s],
                device_id=(db, dl),
                device_id_type=MESH,
            ).start()

        to_peers(crossing_first, one)

    def send_back(s):
        def one(db, dl, d):
            pltpu.make_async_remote_copy(
                src_ref=rs.at[d, :, s],
                dst_ref=back.at[:, my_block, my_group, s],
                send_sem=b_send.at[s],
                recv_sem=b_recv.at[s],
                device_id=(db, dl),
                device_id_type=MESH,
            ).start()

        to_peers(in_turn, one)

    def wait_en(sem, peers, low_slab, count):
        whole = re.at[pl.ds(0, peers), pl.ds(low_slab, count)]
        pltpu.make_async_copy(whole, whole, sem).wait()

    def wait_state(sem, s):
        whole = rs.at[pl.ds(0, others), :, s]
        pltpu.make_async_copy(whole, whole, sem).wait()

    load_turn.wait()
    load_diag.wait()
    scales = []
    for layer in range(LAYERS):
        cosines = []
        for group in range(4):
            angle = jnp.broadcast_to(turn_ref[layer : layer + 1, group : group + 1], (SUB, lanes))
            cosine, sine = cos_sin(angle)
            cosines.append(cosine)
            slope[layer, group] = sine / cosine
        sublane = lax.broadcasted_iota(jnp.int32, (SUB, lanes), 0)
        for place in range(3):
            sign = ((sublane >> place) & 1) * 2 - 1
            signed[layer, place] = slope[layer, 1] * sign.astype(jnp.float32)
        scale = jnp.ones((SUB, lanes), jnp.float32)
        for group, count in ((0, lanes), (1, groups * slabs * rows), (2, blocks * nb), (3, nl)):
            for _ in range(bits_of(count)):
                scale = scale * cosines[group]
        scales.append(scale[0:1, :])
    last[...] = slope[LAYERS - 1, 1]

    def build_table(layer):
        here = lax.broadcasted_iota(jnp.int32, (lanes, lanes), 0)
        there = lax.broadcasted_iota(jnp.int32, (lanes, lanes), 1)
        whole = jnp.broadcast_to(scales[layer], (lanes, lanes))
        tangent = jnp.broadcast_to(slope[layer, 0, 0:1, :], (lanes, lanes))
        for place in range(bits_of(lanes)):
            source, target = (here >> place) & 1, (there >> place) & 1
            sign = (target - source).astype(jnp.float32)
            whole = whole * jnp.where(source == target, 1.0, sign * tangent)
        high = whole.astype(jnp.bfloat16)
        low = (whole - high.astype(jnp.float32)).astype(jnp.bfloat16)
        table[layer, :lanes, :lanes] = high
        table[layer, lanes:, :lanes] = high
        table[layer, :lanes, lanes:] = low
        table[layer, lanes:, lanes:] = jnp.zeros_like(low)

    def over(count, action):
        def step(i, carry):
            action(i)
            return carry

        lax.fori_loop(0, count, step, 0)

    def at_eight(i):
        return pl.ds(pl.multiple_of(i * SUB, SUB), SUB)

    load_amp.wait()
    first_angle = jnp.broadcast_to(diag_ref[0:1, :], (rows, lanes))

    def mix_home(values, mixed, layer, s):
        def one(i):
            part, eight = lax.div(i, eights), at_eight(lax.rem(i, eights))
            pieces = [
                values[part, b, g, s, eight, :] for g in range(groups) for b in range(blocks)
            ]
            inner = bits_of(blocks)
            pieces = turned(pieces, slope[layer, 2], 0, inner)
            pieces = turned(pieces, slope[layer, 1], inner, inner + bits_of(groups))
            for at, piece in enumerate(pieces):
                mixed[part, at % blocks, at // blocks, s, eight, :] = piece

        over(2 * eights, one)

    for s in range(slabs):

        def phase_home(b):
            for g in range(groups):
                cosine, sine = cos_sin(first_angle * en[b, g, s])
                real, imag = amp[0, b, g, s], amp[1, b, g, s]
                amp[0, b, g, s] = real * cosine + imag * sine
                amp[1, b, g, s] = imag * cosine - real * sine

        over(blocks, phase_home)
        mix_home(amp, amp, 0, s)
        if s == 0:
            meet_all()
        send_state(s)
    if slabs > 1:
        send_en(1, slabs - 1, 1, to_unmirrored)
    for part in range(2):
        rs[me, part] = amp[part, my_block, my_group]
    re[me] = en[my_block, my_group]
    for layer in range(LAYERS):
        build_table(layer)

    batch = 8

    def mix_lanes(layer, s):
        def one(i):
            at = pl.ds(i * batch, batch)
            values = rs[at, :, s].reshape(batch * 2 * rows, lanes)
            high = values.astype(jnp.bfloat16)
            low = (values - high.astype(jnp.float32)).astype(jnp.bfloat16)
            both = jnp.dot(
                jnp.concatenate([high, low], axis=1),
                table[layer],
                preferred_element_type=jnp.float32,
            )
            both = both[:, :lanes] + both[:, lanes:]
            rs[at, :, s] = both.reshape(batch, 2, rows, lanes)

        over(devices // batch, one)

    def mix_devices(layer, s):
        def one(part):
            for eight in range(eights):
                pieces = []
                for d in range(devices):
                    piece = rs[d, part, s, eight * SUB : (eight + 1) * SUB, :]
                    sublane = lax.broadcasted_iota(jnp.int32, (SUB, lanes), 0)
                    for place in range(3):
                        step = 1 << place
                        other = pltpu.roll(piece, step, 0)
                        if place < 2:
                            back_roll = pltpu.roll(piece, SUB - step, 0)
                            other = jnp.where((sublane >> place) & 1 == 1, other, back_roll)
                        piece = piece + signed[layer, place] * other
                    pieces.append(piece)
                inner = bits_of(nl)
                pieces = turned(pieces, slope[layer, 3], 0, inner)
                pieces = turned(pieces, slope[layer, 2], inner, inner + bits_of(nb))
                for d in range(devices):
                    rs[d, part, s, eight * SUB : (eight + 1) * SUB, :] = pieces[d]

        over(2, one)

    for s in range(slabs):
        wait_state(s_recv.at[s], s)
        mix_lanes(0, s)
        mix_devices(0, s)

    def slabs_away(d):
        for part in range(2):
            mix_slabs(rs.at[d, part], rs.at[d, part], slope[0, 1])

    over(devices, slabs_away)

    second_angle = jnp.broadcast_to(diag_ref[1:2, :], (rows, lanes))
    for s in range(slabs):
        if s == 0:
            wait_en(e_recv.at[2], mirrored, 0, slabs)
            wait_en(e_recv.at[0], unmirrored, 0, 1)
        if s == 1:
            wait_en(e_recv.at[1], unmirrored, 1, slabs - 1)

        def phase_away(d):
            cosine, sine = cos_sin(second_angle * re[d, s])
            real, imag = rs[d, 0, s], rs[d, 1, s]
            rs[d, 0, s] = real * cosine + imag * sine
            rs[d, 1, s] = imag * cosine - real * sine

        over(devices, phase_away)
        mix_lanes(1, s)
        mix_devices(1, s)
        send_back(s)
    for part in range(2):
        back[part, my_block, my_group] = rs[me, part]

    for s in range(slabs):
        wait_state(b_recv.at[s], s)
        mix_home(back, out, 1, s)

    wait_en(e_send.at[2], mirrored, 0, slabs)
    wait_en(e_send.at[0], unmirrored, 0, 1)
    if slabs > 1:
        wait_en(e_send.at[1], unmirrored, 1, slabs - 1)
    for s in range(slabs):
        wait_state(s_send.at[s], s)
        wait_state(b_send.at[s], s)


def body(nb, nl, amplitudes, energies, diagonal_angles, turn_angles):
    _, blocks, all_rows, lanes = amplitudes.shape
    devices = nb * nl
    groups = devices // blocks
    rows = ROWS_SLAB
    slabs = all_rows // (groups * rows)
    home = (2, blocks, groups, slabs, rows, lanes)
    away = (devices, 2, slabs, rows, lanes)
    grant = VMEM_MOST - 4 * amplitudes.size - ROOM
    dma, regular = pltpu.SemaphoreType.DMA, pltpu.SemaphoreType.REGULAR
    hbm = pl.BlockSpec(memory_space=pl.ANY)
    vmem = pl.BlockSpec(memory_space=pltpu.VMEM)
    values, tangent = pl.pallas_call(
        functools.partial(kernel, nb, nl),
        out_shape=[pltpu.VMEM(home, jnp.float32), pltpu.VMEM((SUB, lanes), jnp.float32)],
        in_specs=[hbm] * 4,
        out_specs=[vmem, vmem],
        scratch_shapes=[
            pltpu.VMEM(home, jnp.float32),
            pltpu.VMEM(home[1:], jnp.float32),
            pltpu.VMEM(diagonal_angles.shape, jnp.float32),
            pltpu.VMEM(turn_angles.shape, jnp.float32),
            pltpu.VMEM(away, jnp.float32),
            pltpu.VMEM((devices,) + away[2:], jnp.float32),
            pltpu.VMEM(home, jnp.float32),
            pltpu.VMEM((LAYERS, 2 * lanes, 2 * lanes), jnp.bfloat16),
            pltpu.VMEM((LAYERS, 4, SUB, lanes), jnp.float32),
            pltpu.VMEM((LAYERS, 3, SUB, lanes), jnp.float32),
            dma((4,)),
            dma((slabs,)),
            dma((slabs,)),
            dma((3,)),
            dma((3,)),
            dma((slabs,)),
            dma((slabs,)),
            regular((bits_of(devices) - 2,)),
            regular,
            regular,
            regular,
            regular,
        ],
        compiler_params=pltpu.CompilerParams(
            collective_id=0, has_side_effects=True, vmem_limit_bytes=grant
        ),
    )(amplitudes.reshape(home), energies.reshape(home[1:]), diagonal_angles, turn_angles)
    out = pl.pallas_call(
        finish,
        out_shape=jax.ShapeDtypeStruct(home, jnp.float32),
        in_specs=[vmem, vmem],
        out_specs=hbm,
        scratch_shapes=[pltpu.VMEM(home, jnp.float32), dma],
        compiler_params=pltpu.CompilerParams(vmem_limit_bytes=32 * 1024 * 1024),
    )(values, tangent)
    return out.reshape(amplitudes.shape)


def solution(mesh):
    placed = (P(None, ("bank", "lane"), None, None), P(("bank", "lane"), None, None), P(), P())
    return jax.shard_map(
        functools.partial(body, mesh.shape["bank"], mesh.shape["lane"]),
        mesh=mesh,
        in_specs=placed,
        out_specs=P(None, ("bank", "lane"), None, None),
        check_vma=False,
    )
```

```python
import functools
import math

import jax
import jax.numpy as jnp
from jax import lax
from jax.experimental import pallas as pl
from jax.experimental.pallas import tpu as pltpu
from jax.sharding import PartitionSpec as P

LAYERS = 2
VMEM_MOST = 67043328
ROOM = 1 << 18
MESH = pl.DeviceIdType.MESH
SUB = 8
ROWS_SLAB = 16


def bits_of(count):
    return count.bit_length() - 1


def xor(number, mask, count):
    out = 0
    for place in range(bits_of(count)):
        weight = 1 << place
        one = lax.rem(lax.div(number, weight), 2) + lax.rem(lax.div(mask, weight), 2)
        out = out + lax.rem(one, 2) * weight
    return out


def flips(number, count):
    out = [number]
    for place in range(bits_of(count)):
        weight = 1 << place
        change = weight - 2 * weight * lax.rem(lax.div(number, weight), 2)
        out = out + [other + change for other in out]
    return out


def cos_sin(turn):
    half = 0.5 * turn
    square = half * half
    sine = jnp.full_like(half, -1.0 / math.factorial(11))
    for power in (9, 7, 5, 3, 1):
        sine = sine * square + (-1.0) ** (power // 2) / math.factorial(power)
    sine = sine * half
    cosine = jnp.full_like(half, -1.0 / math.factorial(10))
    for power in (8, 6, 4, 2, 0):
        cosine = cosine * square + (-1.0) ** (power // 2) / math.factorial(power)
    double = sine + sine
    return 1.0 - double * sine, double * cosine


def turned(pieces, slope, low, high):
    pieces = list(pieces)
    for place in range(low, high):
        step = 1 << place
        for at in range(len(pieces)):
            if not at & step:
                u, v = pieces[at], pieces[at + step]
                pieces[at], pieces[at + step] = u - slope * v, v + slope * u
    return pieces


def mix_slabs(values, mixed, tangent):
    slabs, rows, _ = values.shape
    places = [(s, slice(e, e + SUB)) for s in range(slabs) for e in range(0, rows, SUB)]
    pieces = [values[s, e, :] for s, e in places]
    pieces = turned(pieces, tangent, 0, bits_of(len(places)))
    for (s, e), piece in zip(places, pieces):
        mixed[s, e, :] = piece


def finish(values, tangent, out_hbm, mixed, sem):
    _, blocks, groups, _, _, _ = values.shape

    def one(b, carry):
        for part in range(2):
            for g in range(groups):
                mix_slabs(values.at[part, b, g], mixed.at[part, b, g], tangent[...])
        pltpu.make_async_copy(mixed.at[:, b], out_hbm.at[:, b], sem).start()
        return carry

    lax.fori_loop(0, blocks, one, 0)
    pltpu.make_async_copy(mixed, out_hbm, sem).wait()


def kernel(
    nb, nl, amp_hbm, en_hbm, diag_hbm, turn_hbm, out, last,
    amp, en, diag_ref, turn_ref, rs, re, back, table, slope, signed,
    in_sem, s_send, s_recv, e_send, e_recv, b_send, b_recv, side, outer_in, inner_in, here, all_in,
):
    _, blocks, groups, slabs, rows, lanes = amp.shape
    devices = nb * nl
    others = devices - 1
    eights = rows // SUB
    me_b, me_l = lax.axis_index("bank"), lax.axis_index("lane")
    me = me_b * nl + me_l
    my_block, my_group = lax.rem(me, blocks), lax.div(me, blocks)

    flip_b = flips(me_b, nb)
    flip_l = flips(me_l, nl)

    high, low = nl // 2, nl // 4
    mirror = high + low
    inner = lax.rem(lax.div(me_l, high), 2) != lax.rem(lax.div(me_l, low), 2)
    sides = [(1 << place, 0) for place in range(1, bits_of(nb))]
    sides += [(0, 1 << place) for place in range(bits_of(low))]
    mirrored = devices // 4
    unmirrored = others - mirrored

    def signal(sem, flip):
        pl.semaphore_signal(
            sem, inc=1, device_id=(flip_b[flip[0]], flip_l[flip[1]]), device_id_type=MESH
        )

    def to_unmirrored(action):
        def step(i, carry):
            k = unmirrored - i
            db, dl = xor(me_b, lax.rem(k, nb), nb), xor(me_l, lax.div(k, nb), nl)
            action(db, dl, db * nl + dl)
            return carry

        lax.fori_loop(0, unmirrored, step, 0)

    def to_peers(lane_flips, action):
        for flip in lane_flips:
            far_first = flip - low if flip & low else flip + low
            mine = jnp.where(inner, far_first, flip) if flip & high else flip
            dl = xor(me_l, mine, nl)

            def step(i, carry):
                db = xor(me_b, nb - 1 - i, nb)
                action(db, dl, db * nl + dl)
                return carry

            lax.fori_loop(0, nb if flip else nb - 1, step, 0)

    crossing_first = list(range(nl - 1, -1, -1))
    in_turn = [flip for at in range(high - 1, -1, -1) for flip in (high + at, at)]
    crossing_last = [flip for at in range(high - 1, -1, -1) for flip in (at, high + at)]

    barrier = pltpu.get_barrier_semaphore()

    @pl.when(inner)
    def _():
        for flip in [(0, mirror), (1, mirror)] + sides + [(1, 0), (0, low)]:
            signal(barrier, flip)

    load_en = pltpu.make_async_copy(en_hbm, en, in_sem.at[0])
    load_en.start()
    load_turn = pltpu.make_async_copy(turn_hbm, turn_ref, in_sem.at[2])
    load_turn.start()
    load_diag = pltpu.make_async_copy(diag_hbm, diag_ref, in_sem.at[3])
    load_diag.start()
    load_amp = pltpu.make_async_copy(amp_hbm, amp, in_sem.at[1])
    load_amp.start()

    def send_en(low_slab, count, at, each):
        def one(db, dl, d):
            pltpu.make_async_remote_copy(
                src_ref=en.at[lax.rem(d, blocks), lax.div(d, blocks), pl.ds(low_slab, count)],
                dst_ref=re.at[me, pl.ds(low_slab, count)],
                send_sem=e_send.at[at],
                recv_sem=e_recv.at[at],
                device_id=(db, dl),
                device_id_type=MESH,
            ).start()

        each(one)

    def send_en_mirrored(found):
        def each(action):
            for bank_flip, lane_flip in found:
                db, dl = flip_b[bank_flip], flip_l[lane_flip + mirror]
                action(db, dl, db * nl + dl)

        send_en(0, slabs, 2, each)

    @pl.when(inner)
    def _():
        pl.semaphore_wait(barrier, 3 + len(sides))
        load_en.wait()
        found = [(0, 0), (1, 0)]
        send_en_mirrored(found)
        for at, flip in enumerate(sides):
            signal(side.at[at], flip)
            pl.semaphore_wait(side.at[at], 1)
            more = [(b + flip[0], l + flip[1]) for b, l in found]
            send_en_mirrored(more)
            found += more
        pl.semaphore_wait(outer_in, 1)
        signal(inner_in, (0, low))

    @pl.when(jnp.logical_not(inner))
    def _():
        pl.semaphore_wait(barrier, 1)
        signal(outer_in, (0, low))
        load_en.wait()
        pl.semaphore_wait(inner_in, 1)
        for lane_flip in list(range(high, mirror)) + list(range(low, high)):
            for bank_flip in range(nb):
                signal(here, (bank_flip, lane_flip))

    def meet_all():
        @pl.when(inner)
        def _():
            pl.semaphore_wait(here, devices // 2)
            signal(all_in, (0, low))

        @pl.when(jnp.logical_not(inner))
        def _():
            pl.semaphore_wait(all_in, 1)
            send_en_mirrored([(b, l) for l in range(low) for b in range(nb)])

        send_en(0, 1, 0, to_unmirrored)

    def send_state(s):
        def one(db, dl, d):
            pltpu.make_async_remote_copy(
                src_ref=amp.at[:, lax.rem(d, blocks), lax.div(d, blocks), s],
                dst_ref=rs.at[me, :, s],
                send_sem=s_send.at[s],
                recv_sem=s_recv.at[s],
                device_id=(db, dl),
                device_id_type=MESH,
            ).start()

        to_peers(in_turn, one)

    def send_back(s):
        def one(db, dl, d):
            pltpu.make_async_remote_copy(
                src_ref=rs.at[d, :, s],
                dst_ref=back.at[:, my_block, my_group, s],
                send_sem=b_send.at[s],
                recv_sem=b_recv.at[s],
                device_id=(db, dl),
                device_id_type=MESH,
            ).start()

        to_peers(crossing_last if s == slabs - 1 else crossing_first, one)

    def wait_en(sem, peers, low_slab, count):
        whole = re.at[pl.ds(0, peers), pl.ds(low_slab, count)]
        pltpu.make_async_copy(whole, whole, sem).wait()

    def wait_state(sem, s):
        whole = rs.at[pl.ds(0, others), :, s]
        pltpu.make_async_copy(whole, whole, sem).wait()

    load_turn.wait()
    load_diag.wait()
    scales = []
    for layer in range(LAYERS):
        cosines = []
        for group in range(4):
            angle = jnp.broadcast_to(turn_ref[layer : layer + 1, group : group + 1], (SUB, lanes))
            cosine, sine = cos_sin(angle)
            cosines.append(cosine)
            slope[layer, group] = sine / cosine
        sublane = lax.broadcasted_iota(jnp.int32, (SUB, lanes), 0)
        for place in range(3):
            sign = ((sublane >> place) & 1) * 2 - 1
            signed[layer, place] = slope[layer, 1] * sign.astype(jnp.float32)
        scale = jnp.ones((SUB, lanes), jnp.float32)
        for group, count in ((0, lanes), (1, groups * slabs * rows), (2, blocks * nb), (3, nl)):
            for _ in range(bits_of(count)):
                scale = scale * cosines[group]
        scales.append(scale[0:1, :])
    last[...] = slope[LAYERS - 1, 1]

    def build_table(layer):
        here = lax.broadcasted_iota(jnp.int32, (lanes, lanes), 0)
        there = lax.broadcasted_iota(jnp.int32, (lanes, lanes), 1)
        whole = jnp.broadcast_to(scales[layer], (lanes, lanes))
        tangent = jnp.broadcast_to(slope[layer, 0, 0:1, :], (lanes, lanes))
        for place in range(bits_of(lanes)):
            source, target = (here >> place) & 1, (there >> place) & 1
            sign = (target - source).astype(jnp.float32)
            whole = whole * jnp.where(source == target, 1.0, sign * tangent)
        high = whole.astype(jnp.bfloat16)
        low = (whole - high.astype(jnp.float32)).astype(jnp.bfloat16)
        table[layer, :lanes, :lanes] = high
        table[layer, lanes:, :lanes] = high
        table[layer, :lanes, lanes:] = low
        table[layer, lanes:, lanes:] = jnp.zeros_like(low)

    def over(count, action):
        def step(i, carry):
            action(i)
            return carry

        lax.fori_loop(0, count, step, 0)

    def at_eight(i):
        return pl.ds(pl.multiple_of(i * SUB, SUB), SUB)

    load_amp.wait()
    first_angle = jnp.broadcast_to(diag_ref[0:1, :], (rows, lanes))

    def mix_home(values, mixed, layer, s):
        def one(i):
            part, eight = lax.div(i, eights), at_eight(lax.rem(i, eights))
            pieces = [
                values[part, b, g, s, eight, :] for g in range(groups) for b in range(blocks)
            ]
            inner = bits_of(blocks)
            pieces = turned(pieces, slope[layer, 2], 0, inner)
            pieces = turned(pieces, slope[layer, 1], inner, inner + bits_of(groups))
            for at, piece in enumerate(pieces):
                mixed[part, at % blocks, at // blocks, s, eight, :] = piece

        over(2 * eights, one)

    for s in range(slabs):

        def phase_home(b):
            for g in range(groups):
                cosine, sine = cos_sin(first_angle * en[b, g, s])
                real, imag = amp[0, b, g, s], amp[1, b, g, s]
                amp[0, b, g, s] = real * cosine + imag * sine
                amp[1, b, g, s] = imag * cosine - real * sine

        over(blocks, phase_home)
        mix_home(amp, amp, 0, s)
        if s == 0:
            meet_all()
        send_state(s)
    if slabs > 1:
        send_en(1, slabs - 1, 1, to_unmirrored)
    for part in range(2):
        rs[me, part] = amp[part, my_block, my_group]
    re[me] = en[my_block, my_group]
    for layer in range(LAYERS):
        build_table(layer)

    batch = 8

    def mix_lanes(layer, s):
        def one(i):
            at = pl.ds(i * batch, batch)
            values = rs[at, :, s].reshape(batch * 2 * rows, lanes)
            high = values.astype(jnp.bfloat16)
            low = (values - high.astype(jnp.float32)).astype(jnp.bfloat16)
            both = jnp.dot(
                jnp.concatenate([high, low], axis=1),
                table[layer],
                preferred_element_type=jnp.float32,
            )
            both = both[:, :lanes] + both[:, lanes:]
            rs[at, :, s] = both.reshape(batch, 2, rows, lanes)

        over(devices // batch, one)

    def mix_devices(layer, s):
        def one(part):
            for eight in range(eights):
                pieces = []
                for d in range(devices):
                    piece = rs[d, part, s, eight * SUB : (eight + 1) * SUB, :]
                    sublane = lax.broadcasted_iota(jnp.int32, (SUB, lanes), 0)
                    for place in range(3):
                        step = 1 << place
                        other = pltpu.roll(piece, step, 0)
                        if place < 2:
                            back_roll = pltpu.roll(piece, SUB - step, 0)
                            other = jnp.where((sublane >> place) & 1 == 1, other, back_roll)
                        piece = piece + signed[layer, place] * other
                    pieces.append(piece)
                inner = bits_of(nl)
                pieces = turned(pieces, slope[layer, 3], 0, inner)
                pieces = turned(pieces, slope[layer, 2], inner, inner + bits_of(nb))
                for d in range(devices):
                    rs[d, part, s, eight * SUB : (eight + 1) * SUB, :] = pieces[d]

        over(2, one)

    for s in range(slabs):
        wait_state(s_recv.at[s], s)
        mix_lanes(0, s)
        mix_devices(0, s)

    def slabs_away(d):
        for part in range(2):
            mix_slabs(rs.at[d, part], rs.at[d, part], slope[0, 1])

    over(devices, slabs_away)

    second_angle = jnp.broadcast_to(diag_ref[1:2, :], (rows, lanes))
    for s in range(slabs):
        if s == 0:
            wait_en(e_recv.at[2], mirrored, 0, slabs)
            wait_en(e_recv.at[0], unmirrored, 0, 1)
        if s == 1:
            wait_en(e_recv.at[1], unmirrored, 1, slabs - 1)

        def phase_away(d):
            cosine, sine = cos_sin(second_angle * re[d, s])
            real, imag = rs[d, 0, s], rs[d, 1, s]
            rs[d, 0, s] = real * cosine + imag * sine
            rs[d, 1, s] = imag * cosine - real * sine

        over(devices, phase_away)
        mix_lanes(1, s)
        mix_devices(1, s)
        send_back(s)
    for part in range(2):
        back[part, my_block, my_group] = rs[me, part]

    for s in range(slabs):
        wait_state(b_recv.at[s], s)
        mix_home(back, out, 1, s)

    wait_en(e_send.at[2], mirrored, 0, slabs)
    wait_en(e_send.at[0], unmirrored, 0, 1)
    if slabs > 1:
        wait_en(e_send.at[1], unmirrored, 1, slabs - 1)
    for s in range(slabs):
        wait_state(s_send.at[s], s)
        wait_state(b_send.at[s], s)


def body(nb, nl, amplitudes, energies, diagonal_angles, turn_angles):
    _, blocks, all_rows, lanes = amplitudes.shape
    devices = nb * nl
    groups = devices // blocks
    rows = ROWS_SLAB
    slabs = all_rows // (groups * rows)
    home = (2, blocks, groups, slabs, rows, lanes)
    away = (devices, 2, slabs, rows, lanes)
    grant = VMEM_MOST - 4 * amplitudes.size - ROOM
    dma, regular = pltpu.SemaphoreType.DMA, pltpu.SemaphoreType.REGULAR
    hbm = pl.BlockSpec(memory_space=pl.ANY)
    vmem = pl.BlockSpec(memory_space=pltpu.VMEM)
    values, tangent = pl.pallas_call(
        functools.partial(kernel, nb, nl),
        out_shape=[pltpu.VMEM(home, jnp.float32), pltpu.VMEM((SUB, lanes), jnp.float32)],
        in_specs=[hbm] * 4,
        out_specs=[vmem, vmem],
        scratch_shapes=[
            pltpu.VMEM(home, jnp.float32),
            pltpu.VMEM(home[1:], jnp.float32),
            pltpu.VMEM(diagonal_angles.shape, jnp.float32),
            pltpu.VMEM(turn_angles.shape, jnp.float32),
            pltpu.VMEM(away, jnp.float32),
            pltpu.VMEM((devices,) + away[2:], jnp.float32),
            pltpu.VMEM(home, jnp.float32),
            pltpu.VMEM((LAYERS, 2 * lanes, 2 * lanes), jnp.bfloat16),
            pltpu.VMEM((LAYERS, 4, SUB, lanes), jnp.float32),
            pltpu.VMEM((LAYERS, 3, SUB, lanes), jnp.float32),
            dma((4,)),
            dma((slabs,)),
            dma((slabs,)),
            dma((3,)),
            dma((3,)),
            dma((slabs,)),
            dma((slabs,)),
            regular((bits_of(nb) + bits_of(nl) - 3,)),
            regular,
            regular,
            regular,
            regular,
        ],
        compiler_params=pltpu.CompilerParams(
            collective_id=0, has_side_effects=True, vmem_limit_bytes=grant
        ),
    )(amplitudes.reshape(home), energies.reshape(home[1:]), diagonal_angles, turn_angles)
    out = pl.pallas_call(
        finish,
        out_shape=jax.ShapeDtypeStruct(home, jnp.float32),
        in_specs=[vmem, vmem],
        out_specs=hbm,
        scratch_shapes=[pltpu.VMEM(home, jnp.float32), dma],
        compiler_params=pltpu.CompilerParams(vmem_limit_bytes=32 * 1024 * 1024),
    )(values, tangent)
    return out.reshape(amplitudes.shape)


def solution(mesh):
    placed = (P(None, ("bank", "lane"), None, None), P(("bank", "lane"), None, None), P(), P())
    return jax.shard_map(
        functools.partial(body, mesh.shape["bank"], mesh.shape["lane"]),
        mesh=mesh,
        in_specs=placed,
        out_specs=P(None, ("bank", "lane"), None, None),
        check_vma=False,
    )
```

```python
import functools
import math

import jax
import jax.numpy as jnp
from jax import lax
from jax.experimental import pallas as pl
from jax.experimental.pallas import tpu as pltpu
from jax.sharding import PartitionSpec as P

LAYERS = 2
VMEM_MOST = 67043328
ROOM = 1 << 18
MESH = pl.DeviceIdType.MESH
SUB = 8
ROWS_SLAB = 16


def bits_of(count):
    return count.bit_length() - 1


def xor(number, mask, count):
    out = 0
    for place in range(bits_of(count)):
        weight = 1 << place
        one = lax.rem(lax.div(number, weight), 2) + lax.rem(lax.div(mask, weight), 2)
        out = out + lax.rem(one, 2) * weight
    return out


def flips(number, count):
    out = [number]
    for place in range(bits_of(count)):
        weight = 1 << place
        change = weight - 2 * weight * lax.rem(lax.div(number, weight), 2)
        out = out + [other + change for other in out]
    return out


def cos_sin(turn):
    half = 0.5 * turn
    square = half * half
    sine = jnp.full_like(half, -1.0 / math.factorial(11))
    for power in (9, 7, 5, 3, 1):
        sine = sine * square + (-1.0) ** (power // 2) / math.factorial(power)
    sine = sine * half
    cosine = jnp.full_like(half, -1.0 / math.factorial(10))
    for power in (8, 6, 4, 2, 0):
        cosine = cosine * square + (-1.0) ** (power // 2) / math.factorial(power)
    double = sine + sine
    return 1.0 - double * sine, double * cosine


def turned(pieces, slope, low, high):
    pieces = list(pieces)
    for place in range(low, high):
        step = 1 << place
        for at in range(len(pieces)):
            if not at & step:
                u, v = pieces[at], pieces[at + step]
                pieces[at], pieces[at + step] = u - slope * v, v + slope * u
    return pieces


def mix_slabs(values, mixed, tangent):
    slabs, rows, _ = values.shape
    places = [(s, slice(e, e + SUB)) for s in range(slabs) for e in range(0, rows, SUB)]
    pieces = [values[s, e, :] for s, e in places]
    pieces = turned(pieces, tangent, 0, bits_of(len(places)))
    for (s, e), piece in zip(places, pieces):
        mixed[s, e, :] = piece


def finish(values, tangent, out_hbm, mixed, sem):
    _, blocks, groups, _, _, _ = values.shape

    def one(b, carry):
        for part in range(2):
            for g in range(groups):
                mix_slabs(values.at[part, b, g], mixed.at[part, b, g], tangent[...])
        pltpu.make_async_copy(mixed.at[:, b], out_hbm.at[:, b], sem).start()
        return carry

    lax.fori_loop(0, blocks, one, 0)
    pltpu.make_async_copy(mixed, out_hbm, sem).wait()


def kernel(
    nb, nl, amp_hbm, en_hbm, diag_hbm, turn_hbm, out, last,
    amp, en, diag_ref, turn_ref, rs, re, back, table, slope, signed,
    in_sem, s_send, s_recv, e_send, e_recv, b_send, b_recv, side, outer_in, inner_in, here, all_in,
    en_first, told,
):
    _, blocks, groups, slabs, rows, lanes = amp.shape
    devices = nb * nl
    others = devices - 1
    eights = rows // SUB
    me_b, me_l = lax.axis_index("bank"), lax.axis_index("lane")
    me = me_b * nl + me_l
    my_block, my_group = lax.rem(me, blocks), lax.div(me, blocks)

    flip_b = flips(me_b, nb)
    flip_l = flips(me_l, nl)

    high, low = nl // 2, nl // 4
    mirror = high + low
    inner = lax.rem(lax.div(me_l, high), 2) != lax.rem(lax.div(me_l, low), 2)
    sides = [(1 << place, 0) for place in range(1, bits_of(nb))]
    sides += [(0, 1 << place) for place in range(bits_of(low))]
    mirrored = devices // 4
    unmirrored = others - mirrored

    def signal(sem, flip):
        pl.semaphore_signal(
            sem, inc=1, device_id=(flip_b[flip[0]], flip_l[flip[1]]), device_id_type=MESH
        )

    def to_last(last, count, action):
        def step(i, carry):
            k = last - i
            db, dl = xor(me_b, lax.rem(k, nb), nb), xor(me_l, lax.div(k, nb), nl)
            action(db, dl, db * nl + dl)
            return carry

        lax.fori_loop(0, count, step, 0)

    to_mirrored = functools.partial(to_last, others, mirrored)
    to_unmirrored = functools.partial(to_last, unmirrored, unmirrored)

    def to_peers(lane_flips, action):
        for flip in lane_flips:
            far_first = flip - low if flip & low else flip + low
            mine = jnp.where(inner, far_first, flip) if flip & high else flip
            dl = xor(me_l, mine, nl)

            def step(i, carry):
                db = xor(me_b, nb - 1 - i, nb)
                action(db, dl, db * nl + dl)
                return carry

            lax.fori_loop(0, nb if flip else nb - 1, step, 0)

    crossing_first = list(range(nl - 1, -1, -1))
    in_turn = [flip for at in range(high - 1, -1, -1) for flip in (high + at, at)]
    crossing_last = [flip for at in range(high - 1, -1, -1) for flip in (at, high + at)]

    barrier = pltpu.get_barrier_semaphore()

    upper = jnp.logical_and(inner, lax.div(me_l, high) == 1)
    lower = jnp.logical_and(inner, lax.div(me_l, high) == 0)
    facing = [(0, mirror), (1, mirror)]

    @pl.when(inner)
    def _():
        for flip in facing:
            signal(barrier, flip)

    @pl.when(lower)
    def _():
        for flip in sides + [(1, 0)]:
            signal(barrier, flip)

    def index_of(flip):
        return flip_b[flip[0]] * nl + flip_l[flip[1]]

    @pl.when(inner)
    def _():
        signal(barrier, (0, low))
        for at, flip in enumerate(facing):
            d = index_of(flip)
            pltpu.make_async_copy(
                en_hbm.at[lax.rem(d, blocks), lax.div(d, blocks)], en_first.at[at], in_sem.at[4]
            ).start()

    load_en = pltpu.make_async_copy(en_hbm, en, in_sem.at[0])
    load_en.start()
    load_turn = pltpu.make_async_copy(turn_hbm, turn_ref, in_sem.at[2])
    load_turn.start()
    load_diag = pltpu.make_async_copy(diag_hbm, diag_ref, in_sem.at[3])
    load_diag.start()
    load_amp = pltpu.make_async_copy(amp_hbm, amp, in_sem.at[1])
    load_amp.start()

    def send_en(low_slab, count, at, each):
        def one(db, dl, d):
            pltpu.make_async_remote_copy(
                src_ref=en.at[lax.rem(d, blocks), lax.div(d, blocks), pl.ds(low_slab, count)],
                dst_ref=re.at[me, pl.ds(low_slab, count)],
                send_sem=e_send.at[at],
                recv_sem=e_recv.at[at],
                device_id=(db, dl),
                device_id_type=MESH,
            ).start()

        each(one)

    def send_en_mirrored(found):
        def each(action):
            for bank_flip, lane_flip in found:
                db, dl = flip_b[bank_flip], flip_l[lane_flip + mirror]
                action(db, dl, db * nl + dl)

        send_en(0, slabs, 2, each)

    def send_first():
        pltpu.make_async_copy(en_first, en_first, in_sem.at[4]).wait()
        for at, flip in enumerate(facing):
            pltpu.make_async_remote_copy(
                src_ref=en_first.at[at],
                dst_ref=re.at[me],
                send_sem=e_send.at[2],
                recv_sem=e_recv.at[2],
                device_id=(flip_b[flip[0]], flip_l[flip[1]]),
                device_id_type=MESH,
            ).start()

    near = [(0, 0), (1, 0)]
    single = [(b + flip[0], flip[1]) for flip in sides for b in range(2)]
    every = [(b, l) for l in range(low) for b in range(nb)]

    @pl.when(lower)
    def _():
        pl.semaphore_wait(barrier, 3 + len(sides))
        send_first()
        for flip in facing:
            signal(told.at[0], flip)
        load_en.wait()
        found = list(near)
        for at, flip in enumerate(sides):
            signal(side.at[at], flip)
            pl.semaphore_wait(side.at[at], 1)
            more = [(b + flip[0], l + flip[1]) for b, l in found]
            send_en_mirrored(more)
            found += more
        signal(told.at[1], (0, mirror))

    @pl.when(upper)
    def _():
        pl.semaphore_wait(barrier, 2)
        send_first()
        load_en.wait()
        pl.semaphore_wait(told.at[0], 2)
        send_en_mirrored(single)
        pl.semaphore_wait(told.at[1], 1)
        send_en_mirrored([flip for flip in every if flip not in near + single])

    @pl.when(inner)
    def _():
        pl.semaphore_wait(outer_in, 1)
        signal(inner_in, (0, low))

    @pl.when(jnp.logical_not(inner))
    def _():
        pl.semaphore_wait(barrier, 1)
        signal(outer_in, (0, low))
        load_en.wait()
        pl.semaphore_wait(inner_in, 1)
        for lane_flip in list(range(high, mirror)) + list(range(low, high)):
            for bank_flip in range(nb):
                signal(here, (bank_flip, lane_flip))

    def meet_all():
        @pl.when(inner)
        def _():
            send_state(0, to_mirrored)
            pl.semaphore_wait(here, devices // 2)
            signal(all_in, (0, low))

        @pl.when(jnp.logical_not(inner))
        def _():
            pl.semaphore_wait(all_in, 1)
            send_state(0, to_mirrored)
            send_en_mirrored(every)

        send_en(0, 1, 0, to_unmirrored)
        send_state(0, to_unmirrored)

    def send_state(s, each):
        def one(db, dl, d):
            pltpu.make_async_remote_copy(
                src_ref=amp.at[:, lax.rem(d, blocks), lax.div(d, blocks), s],
                dst_ref=rs.at[me, :, s],
                send_sem=s_send.at[s],
                recv_sem=s_recv.at[s],
                device_id=(db, dl),
                device_id_type=MESH,
            ).start()

        each(one)

    def send_back(s):
        def one(db, dl, d):
            pltpu.make_async_remote_copy(
                src_ref=rs.at[d, :, s],
                dst_ref=back.at[:, my_block, my_group, s],
                send_sem=b_send.at[s],
                recv_sem=b_recv.at[s],
                device_id=(db, dl),
                device_id_type=MESH,
            ).start()

        to_peers(crossing_last if s == slabs - 1 else crossing_first, one)

    def wait_en(sem, peers, low_slab, count):
        whole = re.at[pl.ds(0, peers), pl.ds(low_slab, count)]
        pltpu.make_async_copy(whole, whole, sem).wait()

    def wait_state(sem, s):
        whole = rs.at[pl.ds(0, others), :, s]
        pltpu.make_async_copy(whole, whole, sem).wait()

    load_turn.wait()
    load_diag.wait()
    scales = []
    for layer in range(LAYERS):
        cosines = []
        for group in range(4):
            angle = jnp.broadcast_to(turn_ref[layer : layer + 1, group : group + 1], (SUB, lanes))
            cosine, sine = cos_sin(angle)
            cosines.append(cosine)
            slope[layer, group] = sine / cosine
        sublane = lax.broadcasted_iota(jnp.int32, (SUB, lanes), 0)
        for place in range(3):
            sign = ((sublane >> place) & 1) * 2 - 1
            signed[layer, place] = slope[layer, 1] * sign.astype(jnp.float32)
        scale = jnp.ones((SUB, lanes), jnp.float32)
        for group, count in ((0, lanes), (1, groups * slabs * rows), (2, blocks * nb), (3, nl)):
            for _ in range(bits_of(count)):
                scale = scale * cosines[group]
        scales.append(scale[0:1, :])
    last[...] = slope[LAYERS - 1, 1]

    def build_table(layer):
        here = lax.broadcasted_iota(jnp.int32, (lanes, lanes), 0)
        there = lax.broadcasted_iota(jnp.int32, (lanes, lanes), 1)
        whole = jnp.broadcast_to(scales[layer], (lanes, lanes))
        tangent = jnp.broadcast_to(slope[layer, 0, 0:1, :], (lanes, lanes))
        for place in range(bits_of(lanes)):
            source, target = (here >> place) & 1, (there >> place) & 1
            sign = (target - source).astype(jnp.float32)
            whole = whole * jnp.where(source == target, 1.0, sign * tangent)
        high = whole.astype(jnp.bfloat16)
        low = (whole - high.astype(jnp.float32)).astype(jnp.bfloat16)
        table[layer, :lanes, :lanes] = high
        table[layer, lanes:, :lanes] = high
        table[layer, :lanes, lanes:] = low
        table[layer, lanes:, lanes:] = jnp.zeros_like(low)

    def over(count, action):
        def step(i, carry):
            action(i)
            return carry

        lax.fori_loop(0, count, step, 0)

    def at_eight(i):
        return pl.ds(pl.multiple_of(i * SUB, SUB), SUB)

    load_amp.wait()
    first_angle = jnp.broadcast_to(diag_ref[0:1, :], (rows, lanes))

    def mix_home(values, mixed, layer, s):
        def one(i):
            part, eight = lax.div(i, eights), at_eight(lax.rem(i, eights))
            pieces = [
                values[part, b, g, s, eight, :] for g in range(groups) for b in range(blocks)
            ]
            inner = bits_of(blocks)
            pieces = turned(pieces, slope[layer, 2], 0, inner)
            pieces = turned(pieces, slope[layer, 1], inner, inner + bits_of(groups))
            for at, piece in enumerate(pieces):
                mixed[part, at % blocks, at // blocks, s, eight, :] = piece

        over(2 * eights, one)

    for s in range(slabs):

        def phase_home(b):
            for g in range(groups):
                cosine, sine = cos_sin(first_angle * en[b, g, s])
                real, imag = amp[0, b, g, s], amp[1, b, g, s]
                amp[0, b, g, s] = real * cosine + imag * sine
                amp[1, b, g, s] = imag * cosine - real * sine

        over(blocks, phase_home)
        mix_home(amp, amp, 0, s)
        if s == 0:
            meet_all()
        else:
            send_state(s, functools.partial(to_peers, in_turn))
    if slabs > 1:
        send_en(1, slabs - 1, 1, to_unmirrored)
    for part in range(2):
        rs[me, part] = amp[part, my_block, my_group]
    re[me] = en[my_block, my_group]
    for layer in range(LAYERS):
        build_table(layer)

    batch = 8

    def mix_lanes(layer, s):
        def one(i):
            at = pl.ds(i * batch, batch)
            values = rs[at, :, s].reshape(batch * 2 * rows, lanes)
            high = values.astype(jnp.bfloat16)
            low = (values - high.astype(jnp.float32)).astype(jnp.bfloat16)
            both = jnp.dot(
                jnp.concatenate([high, low], axis=1),
                table[layer],
                preferred_element_type=jnp.float32,
            )
            both = both[:, :lanes] + both[:, lanes:]
            rs[at, :, s] = both.reshape(batch, 2, rows, lanes)

        over(devices // batch, one)

    def mix_devices(layer, s):
        def one(part):
            for eight in range(eights):
                pieces = []
                for d in range(devices):
                    piece = rs[d, part, s, eight * SUB : (eight + 1) * SUB, :]
                    sublane = lax.broadcasted_iota(jnp.int32, (SUB, lanes), 0)
                    for place in range(3):
                        step = 1 << place
                        other = pltpu.roll(piece, step, 0)
                        if place < 2:
                            back_roll = pltpu.roll(piece, SUB - step, 0)
                            other = jnp.where((sublane >> place) & 1 == 1, other, back_roll)
                        piece = piece + signed[layer, place] * other
                    pieces.append(piece)
                inner = bits_of(nl)
                pieces = turned(pieces, slope[layer, 3], 0, inner)
                pieces = turned(pieces, slope[layer, 2], inner, inner + bits_of(nb))
                for d in range(devices):
                    rs[d, part, s, eight * SUB : (eight + 1) * SUB, :] = pieces[d]

        over(2, one)

    for s in range(slabs):
        wait_state(s_recv.at[s], s)
        mix_lanes(0, s)
        mix_devices(0, s)

    def slabs_away(d):
        for part in range(2):
            mix_slabs(rs.at[d, part], rs.at[d, part], slope[0, 1])

    over(devices, slabs_away)

    second_angle = jnp.broadcast_to(diag_ref[1:2, :], (rows, lanes))
    for s in range(slabs):
        if s == 0:
            wait_en(e_recv.at[2], mirrored, 0, slabs)
            wait_en(e_recv.at[0], unmirrored, 0, 1)
        if s == 1:
            wait_en(e_recv.at[1], unmirrored, 1, slabs - 1)

        def phase_away(d):
            cosine, sine = cos_sin(second_angle * re[d, s])
            real, imag = rs[d, 0, s], rs[d, 1, s]
            rs[d, 0, s] = real * cosine + imag * sine
            rs[d, 1, s] = imag * cosine - real * sine

        over(devices, phase_away)
        mix_lanes(1, s)
        mix_devices(1, s)
        send_back(s)
    for part in range(2):
        back[part, my_block, my_group] = rs[me, part]

    for s in range(slabs):
        if s == slabs - 1:
            wait_en(e_send.at[2], mirrored, 0, slabs)
            wait_en(e_send.at[0], unmirrored, 0, 1)
            if slabs > 1:
                wait_en(e_send.at[1], unmirrored, 1, slabs - 1)
            for before in range(slabs):
                wait_state(s_send.at[before], before)
            for before in range(slabs - 1):
                wait_state(b_send.at[before], before)
        wait_state(b_recv.at[s], s)
        mix_home(back, out, 1, s)
    wait_state(b_send.at[slabs - 1], slabs - 1)


def body(nb, nl, amplitudes, energies, diagonal_angles, turn_angles):
    _, blocks, all_rows, lanes = amplitudes.shape
    devices = nb * nl
    groups = devices // blocks
    rows = ROWS_SLAB
    slabs = all_rows // (groups * rows)
    home = (2, blocks, groups, slabs, rows, lanes)
    away = (devices, 2, slabs, rows, lanes)
    grant = VMEM_MOST - 4 * amplitudes.size - ROOM
    dma, regular = pltpu.SemaphoreType.DMA, pltpu.SemaphoreType.REGULAR
    hbm = pl.BlockSpec(memory_space=pl.ANY)
    vmem = pl.BlockSpec(memory_space=pltpu.VMEM)
    values, tangent = pl.pallas_call(
        functools.partial(kernel, nb, nl),
        out_shape=[pltpu.VMEM(home, jnp.float32), pltpu.VMEM((SUB, lanes), jnp.float32)],
        in_specs=[hbm] * 4,
        out_specs=[vmem, vmem],
        scratch_shapes=[
            pltpu.VMEM(home, jnp.float32),
            pltpu.VMEM(home[1:], jnp.float32),
            pltpu.VMEM(diagonal_angles.shape, jnp.float32),
            pltpu.VMEM(turn_angles.shape, jnp.float32),
            pltpu.VMEM(away, jnp.float32),
            pltpu.VMEM((devices,) + away[2:], jnp.float32),
            pltpu.VMEM(home, jnp.float32),
            pltpu.VMEM((LAYERS, 2 * lanes, 2 * lanes), jnp.bfloat16),
            pltpu.VMEM((LAYERS, 4, SUB, lanes), jnp.float32),
            pltpu.VMEM((LAYERS, 3, SUB, lanes), jnp.float32),
            dma((5,)),
            dma((slabs,)),
            dma((slabs,)),
            dma((3,)),
            dma((3,)),
            dma((slabs,)),
            dma((slabs,)),
            regular((bits_of(nb) + bits_of(nl) - 3,)),
            regular,
            regular,
            regular,
            regular,
            pltpu.VMEM((2,) + away[2:], jnp.float32),
            regular((2,)),
        ],
        compiler_params=pltpu.CompilerParams(
            collective_id=0, has_side_effects=True, vmem_limit_bytes=grant
        ),
    )(amplitudes.reshape(home), energies.reshape(home[1:]), diagonal_angles, turn_angles)
    out = pl.pallas_call(
        finish,
        out_shape=jax.ShapeDtypeStruct(home, jnp.float32),
        in_specs=[vmem, vmem],
        out_specs=hbm,
        scratch_shapes=[pltpu.VMEM(home, jnp.float32), dma],
        compiler_params=pltpu.CompilerParams(vmem_limit_bytes=32 * 1024 * 1024),
    )(values, tangent)
    return out.reshape(amplitudes.shape)


def solution(mesh):
    placed = (P(None, ("bank", "lane"), None, None), P(("bank", "lane"), None, None), P(), P())
    return jax.shard_map(
        functools.partial(body, mesh.shape["bank"], mesh.shape["lane"]),
        mesh=mesh,
        in_specs=placed,
        out_specs=P(None, ("bank", "lane"), None, None),
        check_vma=False,
    )
```

```python
import functools
import math

import jax
import jax.numpy as jnp
from jax import lax
from jax.experimental import pallas as pl
from jax.experimental.pallas import tpu as pltpu
from jax.sharding import PartitionSpec as P

LAYERS = 2
VMEM_MOST = 67043328
ROOM = 1 << 18
MESH = pl.DeviceIdType.MESH
SUB = 8
ROWS_SLAB = 16


def bits_of(count):
    return count.bit_length() - 1


def xor(number, mask, count):
    out = 0
    for place in range(bits_of(count)):
        weight = 1 << place
        one = lax.rem(lax.div(number, weight), 2) + lax.rem(lax.div(mask, weight), 2)
        out = out + lax.rem(one, 2) * weight
    return out


def flips(number, count):
    out = [number]
    for place in range(bits_of(count)):
        weight = 1 << place
        change = weight - 2 * weight * lax.rem(lax.div(number, weight), 2)
        out = out + [other + change for other in out]
    return out


def cos_sin(turn):
    half = 0.5 * turn
    square = half * half
    sine = jnp.full_like(half, -1.0 / math.factorial(11))
    for power in (9, 7, 5, 3, 1):
        sine = sine * square + (-1.0) ** (power // 2) / math.factorial(power)
    sine = sine * half
    cosine = jnp.full_like(half, -1.0 / math.factorial(10))
    for power in (8, 6, 4, 2, 0):
        cosine = cosine * square + (-1.0) ** (power // 2) / math.factorial(power)
    double = sine + sine
    return 1.0 - double * sine, double * cosine


def turned(pieces, slope, low, high):
    pieces = list(pieces)
    for place in range(low, high):
        step = 1 << place
        for at in range(len(pieces)):
            if not at & step:
                u, v = pieces[at], pieces[at + step]
                pieces[at], pieces[at + step] = u - slope * v, v + slope * u
    return pieces


def mix_slabs(values, mixed, tangent):
    slabs, rows, _ = values.shape
    places = [(s, slice(e, e + SUB)) for s in range(slabs) for e in range(0, rows, SUB)]
    pieces = [values[s, e, :] for s, e in places]
    pieces = turned(pieces, tangent, 0, bits_of(len(places)))
    for (s, e), piece in zip(places, pieces):
        mixed[s, e, :] = piece


def finish(values, tangent, out_hbm, mixed, sem):
    _, blocks, groups, _, _, _ = values.shape

    def one(b, carry):
        for part in range(2):
            for g in range(groups):
                mix_slabs(values.at[part, b, g], mixed.at[part, b, g], tangent[...])
        pltpu.make_async_copy(mixed.at[:, b], out_hbm.at[:, b], sem).start()
        return carry

    lax.fori_loop(0, blocks, one, 0)
    pltpu.make_async_copy(mixed, out_hbm, sem).wait()


def kernel(
    nb, nl, amp_hbm, en_hbm, diag_hbm, turn_hbm, out, last,
    amp, en, diag_ref, turn_ref, rs, re, back, table, slope, signed,
    in_sem, s_send, s_recv, e_send, e_recv, b_send, b_recv, side, outer_in, inner_in, here, all_in,
    en_first, told,
):
    _, blocks, groups, slabs, rows, lanes = amp.shape
    devices = nb * nl
    others = devices - 1
    eights = rows // SUB
    me_b, me_l = lax.axis_index("bank"), lax.axis_index("lane")
    me = me_b * nl + me_l
    my_block, my_group = lax.rem(me, blocks), lax.div(me, blocks)

    flip_b = flips(me_b, nb)
    flip_l = flips(me_l, nl)

    high, low = nl // 2, nl // 4
    mirror = high + low
    inner = lax.rem(lax.div(me_l, high), 2) != lax.rem(lax.div(me_l, low), 2)
    sides = [(1 << place, 0) for place in range(1, bits_of(nb))]
    sides += [(0, 1 << place) for place in range(bits_of(low))]
    mirrored = devices // 4
    unmirrored = others - mirrored

    def signal(sem, flip):
        pl.semaphore_signal(
            sem, inc=1, device_id=(flip_b[flip[0]], flip_l[flip[1]]), device_id_type=MESH
        )

    def to_last(last, count, action):
        def step(i, carry):
            k = last - i
            db, dl = xor(me_b, lax.rem(k, nb), nb), xor(me_l, lax.div(k, nb), nl)
            action(db, dl, db * nl + dl)
            return carry

        lax.fori_loop(0, count, step, 0)

    to_mirrored = functools.partial(to_last, others, mirrored)
    to_unmirrored = functools.partial(to_last, unmirrored, unmirrored)

    def to_peers(lane_flips, action):
        for flip in lane_flips:
            far_first = flip - low if flip & low else flip + low
            mine = jnp.where(inner, far_first, flip) if flip & high else flip
            dl = xor(me_l, mine, nl)

            def step(i, carry):
                db = xor(me_b, nb - 1 - i, nb)
                action(db, dl, db * nl + dl)
                return carry

            lax.fori_loop(0, nb if flip else nb - 1, step, 0)

    crossing_first = list(range(nl - 1, -1, -1))
    in_turn = [flip for at in range(high - 1, -1, -1) for flip in (high + at, at)]
    crossing_last = [flip for at in range(high - 1, -1, -1) for flip in (at, high + at)]

    barrier = pltpu.get_barrier_semaphore()

    upper = jnp.logical_and(inner, lax.div(me_l, high) == 1)
    lower = jnp.logical_and(inner, lax.div(me_l, high) == 0)
    facing = [(0, mirror), (1, mirror)]

    @pl.when(inner)
    def _():
        for flip in facing:
            signal(barrier, flip)

    @pl.when(lower)
    def _():
        for flip in sides + [(1, 0)]:
            signal(barrier, flip)

    def index_of(flip):
        return flip_b[flip[0]] * nl + flip_l[flip[1]]

    @pl.when(inner)
    def _():
        signal(barrier, (0, low))

    @pl.when(upper)
    def _():
        for at, flip in enumerate(facing):
            d = index_of(flip)
            pltpu.make_async_copy(
                en_hbm.at[lax.rem(d, blocks), lax.div(d, blocks)], en_first.at[at], in_sem.at[4]
            ).start()

    load_en = pltpu.make_async_copy(en_hbm, en, in_sem.at[0])
    load_en.start()
    load_turn = pltpu.make_async_copy(turn_hbm, turn_ref, in_sem.at[2])
    load_turn.start()
    load_diag = pltpu.make_async_copy(diag_hbm, diag_ref, in_sem.at[3])
    load_diag.start()
    load_amp = pltpu.make_async_copy(amp_hbm, amp, in_sem.at[1])
    load_amp.start()

    def send_en(low_slab, count, at, each):
        def one(db, dl, d):
            pltpu.make_async_remote_copy(
                src_ref=en.at[lax.rem(d, blocks), lax.div(d, blocks), pl.ds(low_slab, count)],
                dst_ref=re.at[me, pl.ds(low_slab, count)],
                send_sem=e_send.at[at],
                recv_sem=e_recv.at[at],
                device_id=(db, dl),
                device_id_type=MESH,
            ).start()

        each(one)

    def send_en_mirrored(found):
        def each(action):
            for bank_flip, lane_flip in found:
                db, dl = flip_b[bank_flip], flip_l[lane_flip + mirror]
                action(db, dl, db * nl + dl)

        send_en(0, slabs, 2, each)

    def send_first():
        pltpu.make_async_copy(en_first, en_first, in_sem.at[4]).wait()
        for at, flip in enumerate(facing):
            pltpu.make_async_remote_copy(
                src_ref=en_first.at[at],
                dst_ref=re.at[me],
                send_sem=e_send.at[2],
                recv_sem=e_recv.at[2],
                device_id=(flip_b[flip[0]], flip_l[flip[1]]),
                device_id_type=MESH,
            ).start()

    near = [(0, 0), (1, 0)]
    single = [(b + flip[0], flip[1]) for flip in sides for b in range(2)]
    every = [(b, l) for l in range(low) for b in range(nb)]

    @pl.when(lower)
    def _():
        pl.semaphore_wait(barrier, 3 + len(sides))
        for flip in facing:
            signal(told.at[0], flip)
        load_en.wait()
        send_en_mirrored(near)
        found = list(near)
        for at, flip in enumerate(sides):
            signal(side.at[at], flip)
            pl.semaphore_wait(side.at[at], 1)
            more = [(b + flip[0], l + flip[1]) for b, l in found]
            send_en_mirrored(more)
            found += more
        signal(told.at[1], (0, mirror))

    @pl.when(upper)
    def _():
        pl.semaphore_wait(barrier, 2)
        send_first()
        load_en.wait()
        pl.semaphore_wait(told.at[0], 2)
        send_en_mirrored(single)
        pl.semaphore_wait(told.at[1], 1)
        send_en_mirrored([flip for flip in every if flip not in near + single])

    @pl.when(inner)
    def _():
        pl.semaphore_wait(outer_in, 1)
        signal(inner_in, (0, low))

    @pl.when(jnp.logical_not(inner))
    def _():
        pl.semaphore_wait(barrier, 1)
        signal(outer_in, (0, low))
        load_en.wait()
        pl.semaphore_wait(inner_in, 1)
        for lane_flip in list(range(high, mirror)) + list(range(low, high)):
            for bank_flip in range(nb):
                signal(here, (bank_flip, lane_flip))

    def meet_all():
        @pl.when(inner)
        def _():
            send_state(0, to_mirrored)
            pl.semaphore_wait(here, devices // 2)
            signal(all_in, (0, low))

        @pl.when(jnp.logical_not(inner))
        def _():
            pl.semaphore_wait(all_in, 1)
            send_en_mirrored(every)
            send_state(0, to_mirrored)

        send_state(0, to_unmirrored)
        send_en(0, 1, 0, to_unmirrored)

    def send_state(s, each):
        def one(db, dl, d):
            pltpu.make_async_remote_copy(
                src_ref=amp.at[:, lax.rem(d, blocks), lax.div(d, blocks), s],
                dst_ref=rs.at[me, :, s],
                send_sem=s_send.at[s],
                recv_sem=s_recv.at[s],
                device_id=(db, dl),
                device_id_type=MESH,
            ).start()

        each(one)

    def send_back(s):
        def one(db, dl, d):
            pltpu.make_async_remote_copy(
                src_ref=rs.at[d, :, s],
                dst_ref=back.at[:, my_block, my_group, s],
                send_sem=b_send.at[s],
                recv_sem=b_recv.at[s],
                device_id=(db, dl),
                device_id_type=MESH,
            ).start()

        to_peers(crossing_last if s == slabs - 1 else crossing_first, one)

    def wait_en(sem, peers, low_slab, count):
        whole = re.at[pl.ds(0, peers), pl.ds(low_slab, count)]
        pltpu.make_async_copy(whole, whole, sem).wait()

    def wait_state(sem, s):
        whole = rs.at[pl.ds(0, others), :, s]
        pltpu.make_async_copy(whole, whole, sem).wait()

    load_turn.wait()
    load_diag.wait()
    scales = []
    for layer in range(LAYERS):
        cosines = []
        for group in range(4):
            angle = jnp.broadcast_to(turn_ref[layer : layer + 1, group : group + 1], (SUB, lanes))
            cosine, sine = cos_sin(angle)
            cosines.append(cosine)
            slope[layer, group] = sine / cosine
        sublane = lax.broadcasted_iota(jnp.int32, (SUB, lanes), 0)
        for place in range(3):
            sign = ((sublane >> place) & 1) * 2 - 1
            signed[layer, place] = slope[layer, 1] * sign.astype(jnp.float32)
        scale = jnp.ones((SUB, lanes), jnp.float32)
        for group, count in ((0, lanes), (1, groups * slabs * rows), (2, blocks * nb), (3, nl)):
            for _ in range(bits_of(count)):
                scale = scale * cosines[group]
        scales.append(scale[0:1, :])
    last[...] = slope[LAYERS - 1, 1]

    def build_table(layer):
        here = lax.broadcasted_iota(jnp.int32, (lanes, lanes), 0)
        there = lax.broadcasted_iota(jnp.int32, (lanes, lanes), 1)
        whole = jnp.broadcast_to(scales[layer], (lanes, lanes))
        tangent = jnp.broadcast_to(slope[layer, 0, 0:1, :], (lanes, lanes))
        for place in range(bits_of(lanes)):
            source, target = (here >> place) & 1, (there >> place) & 1
            sign = (target - source).astype(jnp.float32)
            whole = whole * jnp.where(source == target, 1.0, sign * tangent)
        high = whole.astype(jnp.bfloat16)
        low = (whole - high.astype(jnp.float32)).astype(jnp.bfloat16)
        table[layer, :lanes, :lanes] = high
        table[layer, lanes:, :lanes] = high
        table[layer, :lanes, lanes:] = low
        table[layer, lanes:, lanes:] = jnp.zeros_like(low)

    def over(count, action):
        def step(i, carry):
            action(i)
            return carry

        lax.fori_loop(0, count, step, 0)

    def at_eight(i):
        return pl.ds(pl.multiple_of(i * SUB, SUB), SUB)

    load_amp.wait()
    first_angle = jnp.broadcast_to(diag_ref[0:1, :], (rows, lanes))

    def mix_home(values, mixed, layer, s):
        def one(i):
            part, eight = lax.div(i, eights), at_eight(lax.rem(i, eights))
            pieces = [
                values[part, b, g, s, eight, :] for g in range(groups) for b in range(blocks)
            ]
            inner = bits_of(blocks)
            pieces = turned(pieces, slope[layer, 2], 0, inner)
            pieces = turned(pieces, slope[layer, 1], inner, inner + bits_of(groups))
            for at, piece in enumerate(pieces):
                mixed[part, at % blocks, at // blocks, s, eight, :] = piece

        over(2 * eights, one)

    for s in range(slabs):

        def phase_home(b):
            for g in range(groups):
                cosine, sine = cos_sin(first_angle * en[b, g, s])
                real, imag = amp[0, b, g, s], amp[1, b, g, s]
                amp[0, b, g, s] = real * cosine + imag * sine
                amp[1, b, g, s] = imag * cosine - real * sine

        over(blocks, phase_home)
        mix_home(amp, amp, 0, s)
        if s == 0:
            meet_all()
        else:
            send_state(s, functools.partial(to_peers, in_turn))
    if slabs > 1:
        send_en(1, slabs - 1, 1, to_unmirrored)
    for part in range(2):
        rs[me, part] = amp[part, my_block, my_group]
    re[me] = en[my_block, my_group]
    for layer in range(LAYERS):
        build_table(layer)

    batch = 8

    def mix_lanes(layer, s):
        def one(i):
            at = pl.ds(i * batch, batch)
            values = rs[at, :, s].reshape(batch * 2 * rows, lanes)
            high = values.astype(jnp.bfloat16)
            low = (values - high.astype(jnp.float32)).astype(jnp.bfloat16)
            both = jnp.dot(
                jnp.concatenate([high, low], axis=1),
                table[layer],
                preferred_element_type=jnp.float32,
            )
            both = both[:, :lanes] + both[:, lanes:]
            rs[at, :, s] = both.reshape(batch, 2, rows, lanes)

        over(devices // batch, one)

    def mix_devices(layer, s):
        def one(part):
            for eight in range(eights):
                pieces = []
                for d in range(devices):
                    piece = rs[d, part, s, eight * SUB : (eight + 1) * SUB, :]
                    sublane = lax.broadcasted_iota(jnp.int32, (SUB, lanes), 0)
                    for place in range(3):
                        step = 1 << place
                        other = pltpu.roll(piece, step, 0)
                        if place < 2:
                            back_roll = pltpu.roll(piece, SUB - step, 0)
                            other = jnp.where((sublane >> place) & 1 == 1, other, back_roll)
                        piece = piece + signed[layer, place] * other
                    pieces.append(piece)
                inner = bits_of(nl)
                pieces = turned(pieces, slope[layer, 3], 0, inner)
                pieces = turned(pieces, slope[layer, 2], inner, inner + bits_of(nb))
                for d in range(devices):
                    rs[d, part, s, eight * SUB : (eight + 1) * SUB, :] = pieces[d]

        over(2, one)

    for s in range(slabs):
        wait_state(s_recv.at[s], s)
        mix_lanes(0, s)
        mix_devices(0, s)

    def slabs_away(d):
        for part in range(2):
            mix_slabs(rs.at[d, part], rs.at[d, part], slope[0, 1])

    over(devices, slabs_away)

    second_angle = jnp.broadcast_to(diag_ref[1:2, :], (rows, lanes))
    for s in range(slabs):
        if s == 0:
            wait_en(e_recv.at[2], mirrored, 0, slabs)
            wait_en(e_recv.at[0], unmirrored, 0, 1)
        if s == 1:
            wait_en(e_recv.at[1], unmirrored, 1, slabs - 1)

        def phase_away(d):
            cosine, sine = cos_sin(second_angle * re[d, s])
            real, imag = rs[d, 0, s], rs[d, 1, s]
            rs[d, 0, s] = real * cosine + imag * sine
            rs[d, 1, s] = imag * cosine - real * sine

        over(devices, phase_away)
        mix_lanes(1, s)
        mix_devices(1, s)
        send_back(s)
    for part in range(2):
        back[part, my_block, my_group] = rs[me, part]

    for s in range(slabs):
        if s == slabs - 1:
            wait_en(e_send.at[2], mirrored, 0, slabs)
            wait_en(e_send.at[0], unmirrored, 0, 1)
            if slabs > 1:
                wait_en(e_send.at[1], unmirrored, 1, slabs - 1)
            for before in range(slabs):
                wait_state(s_send.at[before], before)
            for before in range(slabs - 1):
                wait_state(b_send.at[before], before)
        wait_state(b_recv.at[s], s)
        mix_home(back, out, 1, s)
    wait_state(b_send.at[slabs - 1], slabs - 1)


def body(nb, nl, amplitudes, energies, diagonal_angles, turn_angles):
    _, blocks, all_rows, lanes = amplitudes.shape
    devices = nb * nl
    groups = devices // blocks
    rows = ROWS_SLAB
    slabs = all_rows // (groups * rows)
    home = (2, blocks, groups, slabs, rows, lanes)
    away = (devices, 2, slabs, rows, lanes)
    grant = VMEM_MOST - 4 * amplitudes.size - ROOM
    dma, regular = pltpu.SemaphoreType.DMA, pltpu.SemaphoreType.REGULAR
    hbm = pl.BlockSpec(memory_space=pl.ANY)
    vmem = pl.BlockSpec(memory_space=pltpu.VMEM)
    values, tangent = pl.pallas_call(
        functools.partial(kernel, nb, nl),
        out_shape=[pltpu.VMEM(home, jnp.float32), pltpu.VMEM((SUB, lanes), jnp.float32)],
        in_specs=[hbm] * 4,
        out_specs=[vmem, vmem],
        scratch_shapes=[
            pltpu.VMEM(home, jnp.float32),
            pltpu.VMEM(home[1:], jnp.float32),
            pltpu.VMEM(diagonal_angles.shape, jnp.float32),
            pltpu.VMEM(turn_angles.shape, jnp.float32),
            pltpu.VMEM(away, jnp.float32),
            pltpu.VMEM((devices,) + away[2:], jnp.float32),
            pltpu.VMEM(home, jnp.float32),
            pltpu.VMEM((LAYERS, 2 * lanes, 2 * lanes), jnp.bfloat16),
            pltpu.VMEM((LAYERS, 4, SUB, lanes), jnp.float32),
            pltpu.VMEM((LAYERS, 3, SUB, lanes), jnp.float32),
            dma((5,)),
            dma((slabs,)),
            dma((slabs,)),
            dma((3,)),
            dma((3,)),
            dma((slabs,)),
            dma((slabs,)),
            regular((bits_of(nb) + bits_of(nl) - 3,)),
            regular,
            regular,
            regular,
            regular,
            pltpu.VMEM((2,) + away[2:], jnp.float32),
            regular((2,)),
        ],
        compiler_params=pltpu.CompilerParams(
            collective_id=0, has_side_effects=True, vmem_limit_bytes=grant
        ),
    )(amplitudes.reshape(home), energies.reshape(home[1:]), diagonal_angles, turn_angles)
    out = pl.pallas_call(
        finish,
        out_shape=jax.ShapeDtypeStruct(home, jnp.float32),
        in_specs=[vmem, vmem],
        out_specs=hbm,
        scratch_shapes=[pltpu.VMEM(home, jnp.float32), dma],
        compiler_params=pltpu.CompilerParams(vmem_limit_bytes=32 * 1024 * 1024),
    )(values, tangent)
    return out.reshape(amplitudes.shape)


def solution(mesh):
    placed = (P(None, ("bank", "lane"), None, None), P(("bank", "lane"), None, None), P(), P())
    return jax.shard_map(
        functools.partial(body, mesh.shape["bank"], mesh.shape["lane"]),
        mesh=mesh,
        in_specs=placed,
        out_specs=P(None, ("bank", "lane"), None, None),
        check_vma=False,
    )
```

```python
import functools
import math

import jax
import jax.numpy as jnp
from jax import lax
from jax.experimental import pallas as pl
from jax.experimental.pallas import tpu as pltpu
from jax.sharding import PartitionSpec as P

LAYERS = 2
VMEM_MOST = 67043328
ROOM = 1 << 18
MESH = pl.DeviceIdType.MESH
SUB = 8
ROWS_SLAB = 16


def bits_of(count):
    return count.bit_length() - 1


def xor(number, mask, count):
    out = 0
    for place in range(bits_of(count)):
        weight = 1 << place
        one = lax.rem(lax.div(number, weight), 2) + lax.rem(lax.div(mask, weight), 2)
        out = out + lax.rem(one, 2) * weight
    return out


def flips(number, count):
    out = [number]
    for place in range(bits_of(count)):
        weight = 1 << place
        change = weight - 2 * weight * lax.rem(lax.div(number, weight), 2)
        out = out + [other + change for other in out]
    return out


def cos_sin(turn):
    half = 0.5 * turn
    square = half * half
    sine = jnp.full_like(half, -1.0 / math.factorial(11))
    for power in (9, 7, 5, 3, 1):
        sine = sine * square + (-1.0) ** (power // 2) / math.factorial(power)
    sine = sine * half
    cosine = jnp.full_like(half, -1.0 / math.factorial(10))
    for power in (8, 6, 4, 2, 0):
        cosine = cosine * square + (-1.0) ** (power // 2) / math.factorial(power)
    double = sine + sine
    return 1.0 - double * sine, double * cosine


def turned(pieces, slope, low, high):
    pieces = list(pieces)
    for place in range(low, high):
        step = 1 << place
        for at in range(len(pieces)):
            if not at & step:
                u, v = pieces[at], pieces[at + step]
                pieces[at], pieces[at + step] = u - slope * v, v + slope * u
    return pieces


def mix_slabs(values, mixed, tangent):
    slabs, rows, _ = values.shape
    places = [(s, slice(e, e + SUB)) for s in range(slabs) for e in range(0, rows, SUB)]
    pieces = [values[s, e, :] for s, e in places]
    pieces = turned(pieces, tangent, 0, bits_of(len(places)))
    for (s, e), piece in zip(places, pieces):
        mixed[s, e, :] = piece


def finish(values, tangent, out_hbm, mixed, sem):
    _, blocks, groups, _, _, _ = values.shape

    def one(b, carry):
        for part in range(2):
            for g in range(groups):
                mix_slabs(values.at[part, b, g], mixed.at[part, b, g], tangent[...])
        pltpu.make_async_copy(mixed.at[:, b], out_hbm.at[:, b], sem).start()
        return carry

    lax.fori_loop(0, blocks, one, 0)
    pltpu.make_async_copy(mixed, out_hbm, sem).wait()


def kernel(
    nb, nl, amp_hbm, en_hbm, diag_hbm, turn_hbm, out, last,
    amp, en, diag_ref, turn_ref, rs, re, back, table, slope, signed,
    in_sem, s_send, s_recv, e_send, e_recv, b_send, b_recv, side, outer_in, inner_in, here, all_in,
    en_first, told,
):
    _, blocks, groups, slabs, rows, lanes = amp.shape
    devices = nb * nl
    others = devices - 1
    eights = rows // SUB
    me_b, me_l = lax.axis_index("bank"), lax.axis_index("lane")
    me = me_b * nl + me_l
    my_block, my_group = lax.rem(me, blocks), lax.div(me, blocks)

    flip_b = flips(me_b, nb)
    flip_l = flips(me_l, nl)

    high, low = nl // 2, nl // 4
    mirror = high + low
    inner = lax.rem(lax.div(me_l, high), 2) != lax.rem(lax.div(me_l, low), 2)
    sides = [(1 << place, 0) for place in range(1, bits_of(nb))]
    sides += [(0, 1 << place) for place in range(bits_of(low))]
    mirrored = devices // 4
    unmirrored = others - mirrored

    def signal(sem, flip):
        pl.semaphore_signal(
            sem, inc=1, device_id=(flip_b[flip[0]], flip_l[flip[1]]), device_id_type=MESH
        )

    def to_last(last, count, action):
        def step(i, carry):
            k = last - i
            db, dl = xor(me_b, lax.rem(k, nb), nb), xor(me_l, lax.div(k, nb), nl)
            action(db, dl, db * nl + dl)
            return carry

        lax.fori_loop(0, count, step, 0)

    to_mirrored = functools.partial(to_last, others, mirrored)
    to_unmirrored = functools.partial(to_last, unmirrored, unmirrored)

    def to_peers(lane_flips, action):
        for flip in lane_flips:
            far_first = flip - low if flip & low else flip + low
            mine = jnp.where(inner, far_first, flip) if flip & high else flip
            dl = xor(me_l, mine, nl)

            def step(i, carry):
                db = xor(me_b, nb - 1 - i, nb)
                action(db, dl, db * nl + dl)
                return carry

            lax.fori_loop(0, nb if flip else nb - 1, step, 0)

    crossing_first = list(range(nl - 1, -1, -1))
    in_turn = [flip for at in range(high - 1, -1, -1) for flip in (high + at, at)]
    crossing_last = [
        side_flip + at - low_flip
        for at in range(high - 1, -1, -2)
        for side_flip in (0, high)
        for low_flip in (0, 1)
    ]

    barrier = pltpu.get_barrier_semaphore()

    upper = jnp.logical_and(inner, lax.div(me_l, high) == 1)
    lower = jnp.logical_and(inner, lax.div(me_l, high) == 0)
    facing = [(0, mirror), (1, mirror)]

    @pl.when(inner)
    def _():
        for flip in facing:
            signal(barrier, flip)

    @pl.when(lower)
    def _():
        for flip in sides + [(1, 0)]:
            signal(barrier, flip)

    def index_of(flip):
        return flip_b[flip[0]] * nl + flip_l[flip[1]]

    @pl.when(inner)
    def _():
        signal(barrier, (0, low))

    @pl.when(upper)
    def _():
        for at, flip in enumerate(facing):
            d = index_of(flip)
            pltpu.make_async_copy(
                en_hbm.at[lax.rem(d, blocks), lax.div(d, blocks)], en_first.at[at], in_sem.at[4]
            ).start()

    load_en = pltpu.make_async_copy(en_hbm, en, in_sem.at[0])
    load_en.start()
    load_turn = pltpu.make_async_copy(turn_hbm, turn_ref, in_sem.at[2])
    load_turn.start()
    load_diag = pltpu.make_async_copy(diag_hbm, diag_ref, in_sem.at[3])
    load_diag.start()
    load_amp = pltpu.make_async_copy(amp_hbm, amp, in_sem.at[1])
    load_amp.start()

    def send_en(low_slab, count, at, each):
        def one(db, dl, d):
            pltpu.make_async_remote_copy(
                src_ref=en.at[lax.rem(d, blocks), lax.div(d, blocks), pl.ds(low_slab, count)],
                dst_ref=re.at[me, pl.ds(low_slab, count)],
                send_sem=e_send.at[at],
                recv_sem=e_recv.at[at],
                device_id=(db, dl),
                device_id_type=MESH,
            ).start()

        each(one)

    def send_en_mirrored(found):
        def each(action):
            for bank_flip, lane_flip in found:
                db, dl = flip_b[bank_flip], flip_l[lane_flip + mirror]
                action(db, dl, db * nl + dl)

        send_en(0, slabs, 2, each)

    def send_first():
        pltpu.make_async_copy(en_first, en_first, in_sem.at[4]).wait()
        for at, flip in enumerate(facing):
            pltpu.make_async_remote_copy(
                src_ref=en_first.at[at],
                dst_ref=re.at[me],
                send_sem=e_send.at[2],
                recv_sem=e_recv.at[2],
                device_id=(flip_b[flip[0]], flip_l[flip[1]]),
                device_id_type=MESH,
            ).start()

    near = [(0, 0), (1, 0)]
    single = [(b + flip[0], flip[1]) for flip in sides for b in range(2)]
    every = [(b, l) for l in range(low) for b in range(nb)]

    @pl.when(lower)
    def _():
        pl.semaphore_wait(barrier, 3 + len(sides))
        for flip in facing:
            signal(told.at[0], flip)
        load_en.wait()
        send_en_mirrored(near)
        found = list(near)
        for at, flip in enumerate(sides):
            signal(side.at[at], flip)
            pl.semaphore_wait(side.at[at], 1)
            more = [(b + flip[0], l + flip[1]) for b, l in found]
            send_en_mirrored(more)
            found += more
        signal(told.at[1], (0, mirror))

    @pl.when(upper)
    def _():
        pl.semaphore_wait(barrier, 2)
        send_first()
        load_en.wait()
        pl.semaphore_wait(told.at[0], 2)
        send_en_mirrored(single)
        pl.semaphore_wait(told.at[1], 1)
        send_en_mirrored([flip for flip in every if flip not in near + single])

    @pl.when(inner)
    def _():
        pl.semaphore_wait(outer_in, 1)
        signal(inner_in, (0, low))

    @pl.when(jnp.logical_not(inner))
    def _():
        pl.semaphore_wait(barrier, 1)
        signal(outer_in, (0, low))
        load_en.wait()
        pl.semaphore_wait(inner_in, 1)
        for lane_flip in list(range(high, mirror)) + list(range(low, high)):
            for bank_flip in range(nb):
                signal(here, (bank_flip, lane_flip))

    def meet_all():
        @pl.when(inner)
        def _():
            send_state(0, to_mirrored)
            pl.semaphore_wait(here, devices // 2)
            signal(all_in, (0, low))

        @pl.when(jnp.logical_not(inner))
        def _():
            pl.semaphore_wait(all_in, 1)
            send_en_mirrored(every)
            send_state(0, to_mirrored)

        send_state(0, to_unmirrored)
        send_en(0, 1, 0, to_unmirrored)

    def send_state(s, each):
        def one(db, dl, d):
            pltpu.make_async_remote_copy(
                src_ref=amp.at[:, lax.rem(d, blocks), lax.div(d, blocks), s],
                dst_ref=rs.at[me, :, s],
                send_sem=s_send.at[s],
                recv_sem=s_recv.at[s],
                device_id=(db, dl),
                device_id_type=MESH,
            ).start()

        each(one)

    def send_back(s):
        def one(db, dl, d):
            pltpu.make_async_remote_copy(
                src_ref=rs.at[d, :, s],
                dst_ref=back.at[:, my_block, my_group, s],
                send_sem=b_send.at[s],
                recv_sem=b_recv.at[s],
                device_id=(db, dl),
                device_id_type=MESH,
            ).start()

        to_peers(crossing_last if s == slabs - 1 else crossing_first, one)

    def wait_en(sem, peers, low_slab, count):
        whole = re.at[pl.ds(0, peers), pl.ds(low_slab, count)]
        pltpu.make_async_copy(whole, whole, sem).wait()

    def wait_state(sem, s):
        whole = rs.at[pl.ds(0, others), :, s]
        pltpu.make_async_copy(whole, whole, sem).wait()

    load_turn.wait()
    load_diag.wait()
    scales = []
    for layer in range(LAYERS):
        cosines = []
        for group in range(4):
            angle = jnp.broadcast_to(turn_ref[layer : layer + 1, group : group + 1], (SUB, lanes))
            cosine, sine = cos_sin(angle)
            cosines.append(cosine)
            slope[layer, group] = sine / cosine
        sublane = lax.broadcasted_iota(jnp.int32, (SUB, lanes), 0)
        for place in range(3):
            sign = ((sublane >> place) & 1) * 2 - 1
            signed[layer, place] = slope[layer, 1] * sign.astype(jnp.float32)
        scale = jnp.ones((SUB, lanes), jnp.float32)
        for group, count in ((0, lanes), (1, groups * slabs * rows), (2, blocks * nb), (3, nl)):
            for _ in range(bits_of(count)):
                scale = scale * cosines[group]
        scales.append(scale[0:1, :])
    last[...] = slope[LAYERS - 1, 1]

    def build_table(layer):
        here = lax.broadcasted_iota(jnp.int32, (lanes, lanes), 0)
        there = lax.broadcasted_iota(jnp.int32, (lanes, lanes), 1)
        whole = jnp.broadcast_to(scales[layer], (lanes, lanes))
        tangent = jnp.broadcast_to(slope[layer, 0, 0:1, :], (lanes, lanes))
        for place in range(bits_of(lanes)):
            source, target = (here >> place) & 1, (there >> place) & 1
            sign = (target - source).astype(jnp.float32)
            whole = whole * jnp.where(source == target, 1.0, sign * tangent)
        high = whole.astype(jnp.bfloat16)
        low = (whole - high.astype(jnp.float32)).astype(jnp.bfloat16)
        table[layer, :lanes, :lanes] = high
        table[layer, lanes:, :lanes] = high
        table[layer, :lanes, lanes:] = low
        table[layer, lanes:, lanes:] = jnp.zeros_like(low)

    def over(count, action):
        def step(i, carry):
            action(i)
            return carry

        lax.fori_loop(0, count, step, 0)

    def at_eight(i):
        return pl.ds(pl.multiple_of(i * SUB, SUB), SUB)

    load_amp.wait()
    first_angle = jnp.broadcast_to(diag_ref[0:1, :], (rows, lanes))

    def mix_home(values, mixed, layer, s):
        def one(i):
            part, eight = lax.div(i, eights), at_eight(lax.rem(i, eights))
            pieces = [
                values[part, b, g, s, eight, :] for g in range(groups) for b in range(blocks)
            ]
            inner = bits_of(blocks)
            pieces = turned(pieces, slope[layer, 2], 0, inner)
            pieces = turned(pieces, slope[layer, 1], inner, inner + bits_of(groups))
            for at, piece in enumerate(pieces):
                mixed[part, at % blocks, at // blocks, s, eight, :] = piece

        over(2 * eights, one)

    for s in range(slabs):

        def phase_home(b):
            for g in range(groups):
                cosine, sine = cos_sin(first_angle * en[b, g, s])
                real, imag = amp[0, b, g, s], amp[1, b, g, s]
                amp[0, b, g, s] = real * cosine + imag * sine
                amp[1, b, g, s] = imag * cosine - real * sine

        over(blocks, phase_home)
        mix_home(amp, amp, 0, s)
        if s == 0:
            meet_all()
        else:
            send_state(s, functools.partial(to_peers, in_turn))
    if slabs > 1:
        send_en(1, slabs - 1, 1, to_unmirrored)
    for part in range(2):
        rs[me, part] = amp[part, my_block, my_group]
    re[me] = en[my_block, my_group]
    for layer in range(LAYERS):
        build_table(layer)

    batch = 8

    def mix_lanes(layer, s):
        def one(i):
            at = pl.ds(i * batch, batch)
            values = rs[at, :, s].reshape(batch * 2 * rows, lanes)
            high = values.astype(jnp.bfloat16)
            low = (values - high.astype(jnp.float32)).astype(jnp.bfloat16)
            both = jnp.dot(
                jnp.concatenate([high, low], axis=1),
                table[layer],
                preferred_element_type=jnp.float32,
            )
            both = both[:, :lanes] + both[:, lanes:]
            rs[at, :, s] = both.reshape(batch, 2, rows, lanes)

        over(devices // batch, one)

    def mix_devices(layer, s):
        def one(part):
            for eight in range(eights):
                pieces = []
                for d in range(devices):
                    piece = rs[d, part, s, eight * SUB : (eight + 1) * SUB, :]
                    sublane = lax.broadcasted_iota(jnp.int32, (SUB, lanes), 0)
                    for place in range(3):
                        step = 1 << place
                        other = pltpu.roll(piece, step, 0)
                        if place < 2:
                            back_roll = pltpu.roll(piece, SUB - step, 0)
                            other = jnp.where((sublane >> place) & 1 == 1, other, back_roll)
                        piece = piece + signed[layer, place] * other
                    pieces.append(piece)
                inner = bits_of(nl)
                pieces = turned(pieces, slope[layer, 3], 0, inner)
                pieces = turned(pieces, slope[layer, 2], inner, inner + bits_of(nb))
                for d in range(devices):
                    rs[d, part, s, eight * SUB : (eight + 1) * SUB, :] = pieces[d]

        over(2, one)

    for s in range(slabs):
        wait_state(s_recv.at[s], s)
        mix_lanes(0, s)
        mix_devices(0, s)

    def slabs_away(d):
        for part in range(2):
            mix_slabs(rs.at[d, part], rs.at[d, part], slope[0, 1])

    over(devices, slabs_away)

    second_angle = jnp.broadcast_to(diag_ref[1:2, :], (rows, lanes))
    for s in range(slabs):
        if s == 0:
            wait_en(e_recv.at[2], mirrored, 0, slabs)
            wait_en(e_recv.at[0], unmirrored, 0, 1)
        if s == 1:
            wait_en(e_recv.at[1], unmirrored, 1, slabs - 1)

        def phase_away(d):
            cosine, sine = cos_sin(second_angle * re[d, s])
            real, imag = rs[d, 0, s], rs[d, 1, s]
            rs[d, 0, s] = real * cosine + imag * sine
            rs[d, 1, s] = imag * cosine - real * sine

        over(devices, phase_away)
        mix_lanes(1, s)
        mix_devices(1, s)
        send_back(s)
    for part in range(2):
        back[part, my_block, my_group] = rs[me, part]

    for s in range(slabs):
        if s == slabs - 1:
            wait_en(e_send.at[2], mirrored, 0, slabs)
            wait_en(e_send.at[0], unmirrored, 0, 1)
            if slabs > 1:
                wait_en(e_send.at[1], unmirrored, 1, slabs - 1)
            for before in range(slabs):
                wait_state(s_send.at[before], before)
            for before in range(slabs - 1):
                wait_state(b_send.at[before], before)
        wait_state(b_recv.at[s], s)
        mix_home(back, out, 1, s)
    wait_state(b_send.at[slabs - 1], slabs - 1)


def body(nb, nl, amplitudes, energies, diagonal_angles, turn_angles):
    _, blocks, all_rows, lanes = amplitudes.shape
    devices = nb * nl
    groups = devices // blocks
    rows = ROWS_SLAB
    slabs = all_rows // (groups * rows)
    home = (2, blocks, groups, slabs, rows, lanes)
    away = (devices, 2, slabs, rows, lanes)
    grant = VMEM_MOST - 4 * amplitudes.size - ROOM
    dma, regular = pltpu.SemaphoreType.DMA, pltpu.SemaphoreType.REGULAR
    hbm = pl.BlockSpec(memory_space=pl.ANY)
    vmem = pl.BlockSpec(memory_space=pltpu.VMEM)
    values, tangent = pl.pallas_call(
        functools.partial(kernel, nb, nl),
        out_shape=[pltpu.VMEM(home, jnp.float32), pltpu.VMEM((SUB, lanes), jnp.float32)],
        in_specs=[hbm] * 4,
        out_specs=[vmem, vmem],
        scratch_shapes=[
            pltpu.VMEM(home, jnp.float32),
            pltpu.VMEM(home[1:], jnp.float32),
            pltpu.VMEM(diagonal_angles.shape, jnp.float32),
            pltpu.VMEM(turn_angles.shape, jnp.float32),
            pltpu.VMEM(away, jnp.float32),
            pltpu.VMEM((devices,) + away[2:], jnp.float32),
            pltpu.VMEM(home, jnp.float32),
            pltpu.VMEM((LAYERS, 2 * lanes, 2 * lanes), jnp.bfloat16),
            pltpu.VMEM((LAYERS, 4, SUB, lanes), jnp.float32),
            pltpu.VMEM((LAYERS, 3, SUB, lanes), jnp.float32),
            dma((5,)),
            dma((slabs,)),
            dma((slabs,)),
            dma((3,)),
            dma((3,)),
            dma((slabs,)),
            dma((slabs,)),
            regular((bits_of(nb) + bits_of(nl) - 3,)),
            regular,
            regular,
            regular,
            regular,
            pltpu.VMEM((2,) + away[2:], jnp.float32),
            regular((2,)),
        ],
        compiler_params=pltpu.CompilerParams(
            collective_id=0, has_side_effects=True, vmem_limit_bytes=grant
        ),
    )(amplitudes.reshape(home), energies.reshape(home[1:]), diagonal_angles, turn_angles)
    out = pl.pallas_call(
        finish,
        out_shape=jax.ShapeDtypeStruct(home, jnp.float32),
        in_specs=[vmem, vmem],
        out_specs=hbm,
        scratch_shapes=[pltpu.VMEM(home, jnp.float32), dma],
        compiler_params=pltpu.CompilerParams(vmem_limit_bytes=32 * 1024 * 1024),
    )(values, tangent)
    return out.reshape(amplitudes.shape)


def solution(mesh):
    placed = (P(None, ("bank", "lane"), None, None), P(("bank", "lane"), None, None), P(), P())
    return jax.shard_map(
        functools.partial(body, mesh.shape["bank"], mesh.shape["lane"]),
        mesh=mesh,
        in_specs=placed,
        out_specs=P(None, ("bank", "lane"), None, None),
        check_vma=False,
    )
```
